32 devices in a mesh: batch: 2 (over x), cy: 4 (over z), cx: 4 (over y, core).
Axes of the slice: x: 2, y: 2, z: 4, core: 2. Of those that a mesh axis runs over, the one named last changes fastest.
Arguments:
- q: bfloat16 [16384, 24, 128], P(('batch', 'cy', 'cx')), parts along dimension 0
- k: bfloat16 [16384, 8, 128], P(('batch', 'cy', 'cx')), parts along dimension 0
- v: bfloat16 [16384, 8, 128], P(('batch', 'cy', 'cx')), parts along dimension 0
Outputs:
- output: bfloat16 [16384, 24, 128], P(('batch', 'cy', 'cx')), parts along dimension 0
There are 2 independent parts. The reference program is written for one: setup_inputs(seed, part) draws one part's arguments, and reference() takes and returns one part's arrays. A program takes and returns all parts, laid end to end along the dimension named above; each array names one.
All inputs are finite; a program needn't handle non-finite values.
Results may differ from the reference program's by a relative error of at most 0.00183193.
Values are sent between devices in bfloat16 or wider.
A program may use at most 1 GiB of HBM per device.

```python
import jax
import jax.numpy as jnp
from jax import lax

HEADS = 24
KV_HEADS = 8
HEAD_DIM = 128
TOK = 512
NDEV = 16
QB = 32

SEQ = NDEV * TOK
CH = TOK // 2
GQ = HEADS // KV_HEADS


def piece_and_position():
    i = jnp.arange(SEQ, dtype=jnp.int32)
    r = i // TOK
    w = i % TOK
    piece = jnp.where(w < CH, r, 2 * NDEV - 1 - r)
    return piece, piece * CH + w % CH


def setup_inputs(seed: int = 0, part: int = 0) -> dict:
    key = jax.random.fold_in(jax.random.key(seed), part)
    kq, kk, kv, ko = jax.random.split(key, 4)
    piece, pos = piece_and_position()
    q = jax.random.normal(kq, (SEQ, HEADS, HEAD_DIM), jnp.float32)
    k = jax.random.normal(kk, (SEQ, KV_HEADS, HEAD_DIM), jnp.float32)
    offs = jax.random.normal(ko, (2 * NDEV, KV_HEADS, HEAD_DIM), jnp.float32)
    v = offs[piece] + 0.5 * jax.random.normal(kv, (SEQ, KV_HEADS, HEAD_DIM), jnp.float32)
    return {'q': q.astype(jnp.bfloat16), 'k': k.astype(jnp.bfloat16), 'v': v.astype(jnp.bfloat16)}


def reference(q, k, v):
    piece, pos = piece_and_position()
    scale = HEAD_DIM ** -0.5
    kf = k.astype(jnp.float32)
    vf = v.astype(jnp.float32)
    qb = q.reshape(SEQ // QB, QB, KV_HEADS, GQ, HEAD_DIM)
    pb = pos.reshape(SEQ // QB, QB)

    def one(xs):
        qi, pi = xs
        s = jnp.einsum('qkgd,skd->kgqs', qi.astype(jnp.float32), kf) * scale
        s = jnp.where(pos[None, :] <= pi[:, None], s, -jnp.inf)
        mx = jnp.max(s, axis=-1, keepdims=True)
        p = jnp.exp(s - mx)
        l = jnp.sum(p, axis=-1)
        o = jnp.einsum('kgqs,skd->qkgd', p.astype(jnp.bfloat16).astype(jnp.float32), vf)
        o = o / jnp.transpose(l, (2, 0, 1))[..., None]
        return o.reshape(QB, HEADS, HEAD_DIM).astype(jnp.bfloat16)

    return lax.map(one, (qb, pb)).reshape(SEQ, HEADS, HEAD_DIM)
```

```python
import functools
import math

import jax
import jax.numpy as jnp
from jax import lax
from jax.experimental import pallas as pl
from jax.experimental.pallas import tpu as pltpu
from jax.sharding import PartitionSpec as P


NX = 4
NZ = 4
SLOTS = 2
GQ = 3
NT = (((1,), (1,)), ((), ()))
MESH = pl.DeviceIdType.MESH
I = jnp.int32


def stage(c, qn, k_ref, v_ref, s_nxt, x_nxt, cur, base):
    rows, tq = k_ref.shape[0], qn.shape[0]
    bk = tq
    if cur is not None:
        s_cur, x_cur, m_ref, l_ref, a_ref = cur
        m0 = m_ref[...]
        m1 = jnp.maximum(m0, jnp.max(x_cur[...], axis=0, keepdims=True))
        al = jnp.exp2((m0 - m1) * c)
        m_ref[...] = m1
        lsum = l_ref[...] * al
    xm = o = None
    for b in range(rows // bk):
        r = slice(b * bk, (b + 1) * bk)
        s = lax.dot_general(k_ref[r, :], qn, NT, preferred_element_type=jnp.float32)
        if base is not None:
            kk = lax.broadcasted_iota(I, s.shape, 0) + b * bk
            qq = lax.broadcasted_iota(I, s.shape, 1) + base
            s = jnp.where(kk <= qq, s, -jnp.inf)
        s_nxt[r, :] = s
        y = jnp.max(s.reshape(bk // 8, 8, tq), axis=0)
        xm = y if xm is None else jnp.maximum(xm, y)
        if cur is not None:
            p = jnp.exp2((s_cur[r, :] - m1) * c)
            lsum = lsum + jnp.sum(p.reshape(bk // 8, 8, tq), axis=0)
            d = jnp.dot(v_ref[:, r], p.astype(jnp.bfloat16), preferred_element_type=jnp.float32)
            o = d if o is None else o + d
    x_nxt[...] = xm
    if cur is not None:
        l_ref[...] = lsum
        a_ref[...] = a_ref[...] * al + o


def unit(c, q_ref, k_ref, v_ref, m_ref, l_ref, a_ref, sa, sb, xa, xb, masked):
    tq = sa.shape[1]
    tiles = q_ref.shape[1] // tq
    n_all = GQ * tiles

    def base(n):
        return lax.rem(I(n), I(tiles)) * tq

    def qt(n):
        return q_ref[lax.div(I(n), I(tiles)), pl.ds(pl.multiple_of(base(n), tq), tq), :]

    def cur(n, s, x):
        return s, x, m_ref.at[n], l_ref.at[n], a_ref.at[n]

    stage(c, qt(0), k_ref, v_ref, sa, xa, None, base(0) if masked else None)

    @pl.loop(0, n_all // 2)
    def _(i):
        n = 2 * i
        stage(c, qt(n + 1), k_ref, v_ref, sb, xb, cur(n, sa, xa), base(n + 1) if masked else None)
        n2 = lax.rem(n + 2, I(n_all))
        stage(c, qt(n2), k_ref, v_ref, sa, xa, cur(n + 1, sb, xb), base(n2) if masked else None)


def kernel(c, q, k, v, o, qb, kb, vb, m, l, a, ost, sa, sb, xa, xb,
           xsend, xrecv, xloc, zrecv, dsend, usend, osend, orecv):
    z = lax.axis_index("cy")
    j = lax.axis_index("cx")
    pc = k.shape[1] // 2
    top = 2 * NZ - 1
    tiles = qb.shape[3] // pc

    def mod(x):
        return lax.rem(x + 2 * NX, I(NX))

    def chunk(part):
        return z if part == 0 else top - z

    def pos(part, jj):
        return jj if part == 0 else NX - 1 - jj

    def span(part, jj):
        return pl.ds(pl.multiple_of(pos(part, jj) * pc, pc), pc)

    barrier = pltpu.get_barrier_semaphore()
    for p in range(1, NX):
        pl.semaphore_signal(barrier, inc=1, device_id={"cx": mod(j + p)}, device_id_type=MESH)

    @pl.when(z > 0)
    def _():
        pl.semaphore_signal(barrier, inc=1, device_id={"cy": z - 1}, device_id_type=MESH)

    @pl.when(z < NZ - 1)
    def _():
        pl.semaphore_signal(barrier, inc=1, device_id={"cy": z + 1}, device_id_type=MESH)

    pl.semaphore_wait(barrier, NX - 1 + jnp.where(z > 0, 1, 0) + jnp.where(z < NZ - 1, 1, 0))

    def pair(g, kind, part, owner, dest):
        half = pl.ds(part * pc, pc)
        at = span(part, owner)
        if kind == 0:
            return k.at[SLOTS * dest + g, half, :], kb.at[g, chunk(part), at, :]
        if kind == 1:
            return v.at[SLOTS * dest + g, :, half], vb.at[g, chunk(part), :, at]
        return q.at[pl.ds(GQ * (SLOTS * dest + g), GQ), half, :], qb.at[g, part, :, at, :]

    def xcopy(g, kind, part, p, owner, dest):
        src, dst = pair(g, kind, part, owner, dest)
        return pltpu.make_async_remote_copy(
            src_ref=src, dst_ref=dst, send_sem=xsend.at[g, kind, part, p - 1], recv_sem=xrecv.at[g, kind, part, p - 1],
            device_id={"cx": dest}, device_id_type=MESH)

    def xlocal(g, kind, part):
        src, dst = pair(g, kind, part, j, j)
        return pltpu.make_async_copy(src, dst, xloc.at[g, kind, part])

    def xwait(g, kinds):
        for kind in kinds:
            for part in range(2):
                xlocal(g, kind, part).wait()
                for p in range(1, NX):
                    xcopy(g, kind, part, p, mod(j - p), j).wait_recv()

    for g in range(SLOTS):
        for kinds in ((0, 1), (2,)):
            for p in range(1, NX):
                for kind in kinds:
                    for part in range(2):
                        xcopy(g, kind, part, p, j, mod(j + p)).start()
            for kind in kinds:
                for part in range(2):
                    xlocal(g, kind, part).start()

    def zcopies(g, ch, dz, send):
        return [
            pltpu.make_async_remote_copy(
                src_ref=buf.at[g, ch], dst_ref=buf.at[g, ch], send_sem=send.at[g, ch, i], recv_sem=zrecv.at[g, ch, i],
                device_id={"cy": z + dz}, device_id_type=MESH)
            for i, buf in enumerate((kb, vb))
        ]

    def down(g, ch):
        @pl.when(z > 0)
        def _():
            for d in zcopies(g, ch, -1, dsend):
                d.start()

    def up(g, ch):
        @pl.when(z < NZ - 1)
        def _():
            for d in zcopies(g, ch, 1, usend):
                d.start()

    m[...] = jnp.full_like(m, -jnp.inf)
    l[...] = jnp.zeros_like(l)

    @pl.loop(0, SLOTS * 2)
    def _(i):
        a[lax.div(i, I(2)), lax.rem(i, I(2))] = jnp.zeros(a.shape[2:], a.dtype)

    def run(g, qc, ch, masked):
        unit(c, qb.at[g, qc], kb.at[g, ch], vb.at[g, ch], m.at[g, qc], l.at[g, qc], a.at[g, qc], sa, sb, xa, xb, masked)

    def ocopy(g, part, p, owner, dest):
        return pltpu.make_async_remote_copy(
            src_ref=ost.at[g, part, :, span(part, dest), :],
            dst_ref=o.at[pl.ds(GQ * (SLOTS * owner + g), GQ), pl.ds(part * pc, pc), :],
            send_sem=osend.at[g, part, p], recv_sem=orecv.at[g, part, p - 1],
            device_id={"cx": dest}, device_id_type=MESH)

    def olocal(g, part):
        return pltpu.make_async_copy(
            ost.at[g, part, :, span(part, j), :], o.at[pl.ds(GQ * (SLOTS * j + g), GQ), pl.ds(part * pc, pc), :],
            osend.at[g, part, 0])

    @pl.loop(0, NZ * SLOTS)
    def _(step):
        t = lax.div(step, I(SLOTS))
        g = lax.rem(step, I(SLOTS))
        below = (t > 0) & (z >= t)
        above = (t > 0) & (z + t < NZ)

        @pl.when(t == 0)
        def _():
            xwait(g, (0, 1))
            for ch in (z, top - z):
                down(g, ch)
            up(g, z)
            xwait(g, (2,))

            @pl.loop(0, 2)
            def _(qc):
                run(g, qc, jnp.where(qc == 0, z, top - z), True)

        nb = jnp.where(below, 2, 0)
        nu = jnp.where(t == 0, 1, nb + jnp.where(above, 2, 0))

        @pl.loop(0, nu)
        def _(u):
            is_below = u < nb
            s = z + t
            ch = jnp.where(t == 0, z, jnp.where(is_below, z - t, jnp.where(u == nb, s, top - s)))
            qc = jnp.where(is_below, u, 1)

            @pl.when(is_below & (u == 0))
            def _():
                for d in zcopies(g, ch, 1, usend):
                    d.wait_recv()
                up(g, ch)

            @pl.when((t > 0) & (u >= nb))
            def _():
                for d in zcopies(g, ch, -1, dsend):
                    d.wait_recv()
                down(g, ch)

            run(g, qc, ch, False)

        @pl.when(t == NZ - 1)
        def _():
            for part in range(2):
                @pl.loop(0, GQ * tiles)
                def _(n):
                    y = a[g, part, n] / jnp.sum(l[g, part, n], axis=0, keepdims=True)
                    at = pl.ds(pl.multiple_of(lax.rem(n, I(tiles)) * pc, pc), pc)
                    ost[g, part, lax.div(n, I(tiles)), at, :] = y.T.astype(ost.dtype)
            for part in range(2):
                for p in range(1, NX):
                    ocopy(g, part, p, j, mod(j + p)).start()
                olocal(g, part).start()

    for g in range(SLOTS):
        for part in range(2):
            olocal(g, part).wait()
            for p in range(1, NX):
                ocopy(g, part, p, mod(j - p), j).wait_recv()
                ocopy(g, part, p, j, mod(j + p)).wait_send()
                for kind in range(3):
                    xcopy(g, kind, part, p, j, mod(j + p)).wait_send()
        for s in range(NZ):
            @pl.when((z > 0) & (s >= z))
            def _():
                for ch in (s, top - s):
                    for d in zcopies(g, ch, -1, dsend):
                        d.wait_send()

            @pl.when((z < NZ - 1) & (s <= z))
            def _():
                for d in zcopies(g, s, 1, usend):
                    d.wait_send()


def solution(mesh):
    assert mesh.shape["cx"] == NX and mesh.shape["cy"] == NZ
    spec = P(("batch", "cy", "cx"), None, None)

    def local(q, k, v):
        t, h, d = q.shape
        pc = t // 2
        rows = NX * pc
        c = d ** -0.5 * math.log2(math.e)
        tiles = rows // pc
        f32, bf = jnp.float32, jnp.bfloat16
        dma = pltpu.SemaphoreType.DMA
        ot = pl.pallas_call(
            functools.partial(kernel, c),
            out_shape=jax.ShapeDtypeStruct((h, t, d), bf),
            in_specs=[pl.BlockSpec(memory_space=pl.ANY)] * 3,
            out_specs=pl.BlockSpec(memory_space=pl.ANY),
            scratch_shapes=[
                pltpu.VMEM((SLOTS, 2, GQ, rows, d), bf),
                pltpu.VMEM((SLOTS, 2 * NZ, rows, d), bf),
                pltpu.VMEM((SLOTS, 2 * NZ, d, rows), bf),
                pltpu.VMEM((SLOTS, 2, GQ * tiles, 1, pc), f32),
                pltpu.VMEM((SLOTS, 2, GQ * tiles, 8, pc), f32),
                pltpu.VMEM((SLOTS, 2, GQ * tiles, d, pc), f32),
                pltpu.VMEM((SLOTS, 2, GQ, rows, d), bf),
                pltpu.VMEM((rows, pc), f32),
                pltpu.VMEM((rows, pc), f32),
                pltpu.VMEM((8, pc), f32),
                pltpu.VMEM((8, pc), f32),
                dma((SLOTS, 3, 2, NX - 1)),
                dma((SLOTS, 3, 2, NX - 1)),
                dma((SLOTS, 3, 2)),
                dma((SLOTS, 2 * NZ, 2)),
                dma((SLOTS, 2 * NZ, 2)),
                dma((SLOTS, 2 * NZ, 2)),
                dma((SLOTS, 2, NX)),
                dma((SLOTS, 2, NX - 1)),
            ],
            compiler_params=pltpu.CompilerParams(
                collective_id=0, has_side_effects=True, vmem_limit_bytes=56 * 2**20),
        )(jnp.transpose(q, (1, 0, 2)), jnp.transpose(k, (1, 0, 2)), jnp.transpose(v, (1, 2, 0)))
        return jnp.transpose(ot, (1, 0, 2))

    return jax.shard_map(local, mesh=mesh, in_specs=(spec, spec, spec), out_specs=spec, check_vma=False)
```

```python
import functools
import math

import jax
import jax.numpy as jnp
from jax import lax
from jax.experimental import pallas as pl
from jax.experimental.pallas import tpu as pltpu
from jax.sharding import PartitionSpec as P


NX = 4
NZ = 4
SLOTS = 2
GQ = 3
NB = 4
NT = (((1,), (1,)), ((), ()))
MESH = pl.DeviceIdType.MESH
I = jnp.int32


def stage(c, nxt, cur):
    qn, kn_ref, s_nxt, x_nxt, base = nxt
    rows, tq = kn_ref.shape[0], qn.shape[0]
    bk = rows // NB
    if cur is not None:
        s_cur, x_cur, v_ref, m_ref, l_ref, a_ref = cur
        m0 = m_ref[...]
        m1 = jnp.maximum(m0, jnp.max(x_cur[...], axis=0, keepdims=True))
        al = jnp.exp2((m0 - m1) * c)
        m_ref[...] = m1
        lsum = l_ref[...] * al
    xm = o = None
    for b in range(rows // bk):
        r = slice(b * bk, (b + 1) * bk)
        s = lax.dot_general(kn_ref[r, :], qn, NT, preferred_element_type=jnp.float32)
        if base is not None:
            kk = lax.broadcasted_iota(I, s.shape, 0) + b * bk
            qq = lax.broadcasted_iota(I, s.shape, 1) + base
            s = jnp.where(kk <= qq, s, -jnp.inf)
        s_nxt[r, :] = s
        y = jnp.max(s.reshape(bk // 8, 8, tq), axis=0)
        xm = y if xm is None else jnp.maximum(xm, y)
        if cur is not None:
            p = jnp.exp2((s_cur[r, :] - m1) * c)
            lsum = lsum + jnp.sum(p.reshape(bk // 8, 8, tq), axis=0)
            d = jnp.dot(v_ref[:, r], p.astype(jnp.bfloat16), preferred_element_type=jnp.float32)
            o = d if o is None else o + d
    x_nxt[...] = xm
    if cur is not None:
        l_ref[...] = lsum
        a_ref[...] = a_ref[...] * al + o


SHIFT = 4
TOP = 2 * NZ - 1
START, EXTRA, BELOW, ABOVE = 1, 2, 3, 4


def units(z):
    out = []
    for g in range(SLOTS):
        has_high = not (z == 0 and g == 1)
        out.append((2 * g, g, z, 1, START))
        if has_high:
            out.append((2 * g + 1, g, TOP - z, 1, 0))
            out.append((2 * g + 1, g, z, 0, 0))
    if z == 1:
        out += [(SHIFT, 1, TOP, 1, EXTRA), (SHIFT, 1, z, 0, 0), (SHIFT, 1, TOP - z, 0, 0)]
    for t in range(1, NZ):
        for g in range(SLOTS):
            extra = z == 1 and g == 1
            if z >= t:
                s = z - t
                out.append((2 * g, g, s, 0, BELOW))
                if extra:
                    out.append((SHIFT, g, s, 0, 0))
                out.append((2 * g + 1, g, s, 0, 0))
            if z + t < NZ and not (z == 0 and g == 1):
                for ch in (z + t, TOP - z - t):
                    if extra:
                        out.append((SHIFT, g, ch, 0, ABOVE))
                    out.append((2 * g + 1, g, ch, 0, 0 if extra else ABOVE))
    last = {u[0]: i for i, u in enumerate(out)}
    return [u + (int(last[u[0]] == i),) for i, u in enumerate(out)]


RADIX = (5, 2, 8, 2, 5, 2)


def pack(u):
    x = 0
    for r, f in zip(RADIX, u):
        x = x * r + f
    return x


def unpack(x):
    out = []
    for r in RADIX[::-1]:
        out.append(lax.rem(x, I(r)))
        x = lax.div(x, I(r))
    return out[::-1]


def kernel(c, q, k, v, o, qb, kb, vb, m, l, a, ost, sa, sb, xa, xb,
           xsend, xrecv, xloc, zrecv, dsend, usend, osend, orecv):
    z = lax.axis_index("cy")
    j = lax.axis_index("cx")
    pc = k.shape[1] // 2
    tq = sa.shape[1]
    tiles = qb.shape[2] // tq
    n_all = GQ * tiles

    def mod(x):
        return lax.rem(x + 2 * NX, I(NX))

    def chunk(part):
        return z if part == 0 else TOP - z

    def pos(part, jj):
        return jj if part == 0 else NX - 1 - jj

    def span(part, jj):
        return pl.ds(pl.multiple_of(pos(part, jj) * pc, pc), pc)

    barrier = pltpu.get_barrier_semaphore()
    for p in range(1, NX):
        pl.semaphore_signal(barrier, inc=1, device_id={"cx": mod(j + p)}, device_id_type=MESH)

    @pl.when(z > 0)
    def _():
        pl.semaphore_signal(barrier, inc=1, device_id={"cy": z - 1}, device_id_type=MESH)

    @pl.when(z < NZ - 1)
    def _():
        pl.semaphore_signal(barrier, inc=1, device_id={"cy": z + 1}, device_id_type=MESH)

    @pl.when(z < 2)
    def _():
        for p in range(1, NX):
            pl.semaphore_signal(barrier, inc=1, device_id={"cy": 1 - z, "cx": mod(j + p)}, device_id_type=MESH)

    def by_z(values):
        x = I(values[-1])
        for zz in range(NZ - 1):
            x = jnp.where(z == zz, I(values[zz]), x)
        return x

    lists = [[pack(u) for u in units(zz)] for zz in range(NZ)]
    count = by_z([len(x) for x in lists])
    codes = [by_z([x[min(i, len(x) - 1)] for x in lists]) for i in range(max(map(len, lists)))]

    def fields(u):
        x = codes[-1]
        for i, code in enumerate(codes[:-1]):
            x = jnp.where(u == i, code, x)
        return unpack(x)

    pl.semaphore_wait(
        barrier, NX - 1 + jnp.where(z > 0, 1, 0) + jnp.where(z < NZ - 1, 1, 0) + jnp.where(z < 2, NX - 1, 0))

    def pair(g, kind, part, e, owner, dest):
        half = pl.ds(part * pc, pc)
        at = span(part, owner)
        ch = I(TOP) if e == 2 else chunk(part)
        if kind == 0:
            return k.at[SLOTS * dest + g, half, :], kb.at[g, ch, at, :]
        if kind == 1:
            return v.at[SLOTS * dest + g, :, half], vb.at[g, ch, :, at]
        qs = SHIFT if e == 2 else 2 * g + part
        return q.at[pl.ds(GQ * (SLOTS * dest + g), GQ), half, :], qb.at[qs, :, at, :]

    def xcopy(g, kind, part, p, owner, dest, shifted=False):
        e = 2 if shifted else part
        src, dst = pair(g, kind, part, e, owner, dest)
        return pltpu.make_async_remote_copy(
            src_ref=src, dst_ref=dst, send_sem=xsend.at[g, kind, part, p], recv_sem=xrecv.at[g, kind, e, p],
            device_id={"cy": I(1) if shifted else z, "cx": dest}, device_id_type=MESH)

    def xlocal(g, kind, part):
        src, dst = pair(g, kind, part, part, j, j)
        return pltpu.make_async_copy(src, dst, xloc.at[g, kind, part])

    def xpart(g, part, fn, moved):
        if g == 1 and part == 1:
            pl.when(z == 0)(moved)
            pl.when(z > 0)(fn)
        else:
            fn()

    for g in range(SLOTS):
        for kinds in ((0, 1), (2,)):
            for part in range(2):
                def keep():
                    for p in range(1, NX):
                        for kind in kinds:
                            xcopy(g, kind, part, p, j, mod(j + p)).start()
                    for kind in kinds:
                        xlocal(g, kind, part).start()

                def give():
                    for p in range(NX):
                        for kind in kinds:
                            xcopy(g, kind, part, p, j, mod(j + p), True).start()

                xpart(g, part, keep, give)

    def xwait(g, kinds):
        for part in range(2):
            def keep():
                for kind in kinds:
                    xlocal(g, kind, part).wait()
                    for p in range(1, NX):
                        xcopy(g, kind, part, p, mod(j - p), j).wait_recv()

            xpart(g, part, keep, lambda: None)

    def zcopies(g, ch, dz, send):
        return [
            pltpu.make_async_remote_copy(
                src_ref=buf.at[g, ch], dst_ref=buf.at[g, ch], send_sem=send.at[g, ch, i], recv_sem=zrecv.at[g, ch, i],
                device_id={"cy": z + dz}, device_id_type=MESH)
            for i, buf in enumerate((kb, vb))
        ]

    def goes_down(g):
        return z > jnp.where(g == 1, 1, 0)

    def down(g, ch):
        @pl.when(goes_down(g))
        def _():
            for d in zcopies(g, ch, -1, dsend):
                d.start()

    def up(g, ch):
        @pl.when(z < NZ - 1)
        def _():
            for d in zcopies(g, ch, 1, usend):
                d.start()

    m[...] = jnp.full_like(m, -jnp.inf)
    l[...] = jnp.zeros_like(l)

    @pl.loop(0, 5)
    def _(i):
        a[i] = jnp.zeros(a.shape[1:], a.dtype)

    def before(f):
        _, g, ch, _, act, _ = f
        for gg in range(SLOTS):
            @pl.when((act == START) & (g == gg))
            def _():
                xwait(gg, (0, 1))
                down(I(gg), z)
                up(I(gg), z)
                pl.when(z > 0)(lambda: down(I(gg), TOP - z))
                xwait(gg, (2,))

        @pl.when(act == EXTRA)
        def _():
            for kind in range(3):
                for p in range(NX):
                    xcopy(1, kind, 1, p, mod(j - p), j, True).wait_recv()

        @pl.when(act == BELOW)
        def _():
            for d in zcopies(g, ch, 1, usend):
                d.wait_recv()
            up(g, ch)

        @pl.when(act == ABOVE)
        def _():
            for d in zcopies(g, ch, -1, dsend):
                d.wait_recv()
            down(g, ch)

    def opiece(g, part, p, owner, dest, heads, hd, shifted):
        qs = SHIFT if shifted else 2 * g + part
        return dict(
            src_ref=ost.at[qs, pl.ds(hd, heads), span(part, dest), :],
            dst_ref=o.at[pl.ds(GQ * (SLOTS * owner + g) + hd, heads), pl.ds(part * pc, pc), :])

    def oremote(g, part, p, owner, dest, heads=GQ, hd=0, shifted=False):
        return pltpu.make_async_remote_copy(
            **opiece(g, part, p, owner, dest, heads, hd, shifted),
            send_sem=osend.at[SHIFT if shifted else 2 * g + part, p], recv_sem=orecv.at[2 * g + part, p],
            device_id={"cy": I(0) if shifted else z, "cx": dest}, device_id_type=MESH)

    def olocal(g, part, heads=GQ, hd=0):
        r = opiece(g, part, 0, j, j, heads, hd, False)
        return pltpu.make_async_copy(r["src_ref"], r["dst_ref"], osend.at[2 * g + part, 0])

    def finish(qs, n):
        y = a[qs, n] / jnp.sum(l[qs, n], axis=0, keepdims=True)
        at = pl.ds(pl.multiple_of(lax.rem(n, I(tiles)) * tq, tq), tq)
        ost[qs, lax.div(n, I(tiles)), at, :] = y.astype(ost.dtype).T

    def give_back(qs, n):
        hd = lax.div(n, I(tiles))
        for case in range(5):
            @pl.when(qs == case)
            def _():
                shifted = case == SHIFT
                g, part = (1, 1) if shifted else (case // 2, case % 2)
                for e in range(tq // pc):
                    at = lax.rem(n, I(tiles)) * (tq // pc) + e
                    dest = pos(part, at)
                    p = mod(dest - j)
                    if shifted:
                        oremote(g, part, p, j, dest, 1, hd, True).start()
                    else:
                        pl.when(p == 0)(lambda: olocal(g, part, 1, hd).start())
                        pl.when(p > 0)(lambda: oremote(g, part, p, j, dest, 1, hd).start())

    def after(f, w, n):
        pl.when(f[5] == 1)(lambda: finish(f[0], n))
        pl.when(w[5] == 1)(lambda: give_back(w[0], lax.rem(n + n_all - 1, I(n_all))))

    def nxt(f, n, s, x, masked):
        base = lax.rem(I(n), I(tiles)) * tq
        at = pl.ds(pl.multiple_of(base, tq), tq)
        return qb[f[0], lax.div(I(n), I(tiles)), at, :], kb.at[f[1], f[2]], s, x, base if masked else None

    def step(fn, nn, s_n, x_n, f, n, s_c, x_c):
        qs = f[0]
        for masked in (False, True):
            @pl.when(fn[3] == int(masked))
            def _():
                stage(c, nxt(fn, nn, s_n, x_n, masked),
                      (s_c, x_c, vb.at[f[1], f[2]], m.at[qs, n], l.at[qs, n], a.at[qs, n]))

    first = fields(I(0))
    before(first)
    stage(c, nxt(first, 0, sa, xa, True), None)

    @pl.loop(0, count)
    def _(u):
        f = fields(u)
        fn = fields(jnp.minimum(u + 1, count - 1))
        w = fields(jnp.maximum(u - 1, 0))
        w[5] = jnp.where(u > 0, w[5], 0)

        @pl.loop(0, n_all // 2)
        def _(i):
            n = 2 * i
            step(f, n + 1, sb, xb, f, n, sa, xa)
            after(f, [jnp.where(i == 0, p, q) for p, q in zip(w, f)], n)
            wrap = i == n_all // 2 - 1
            pl.when(wrap & (u + 1 < count))(lambda: before(fn))
            step([jnp.where(wrap, p, q) for p, q in zip(fn, f)], jnp.where(wrap, 0, n + 2), sa, xa, f, n + 1, sb, xb)
            after(f, f, n + 1)

    for g in range(SLOTS):
        for part in range(2):
            def keep():
                for p in range(1, NX):
                    for kind in range(3):
                        xcopy(g, kind, part, p, j, mod(j + p)).wait_send()

            def give():
                for p in range(NX):
                    for kind in range(3):
                        xcopy(g, kind, part, p, j, mod(j + p), True).wait_send()

            xpart(g, part, keep, give)
    give_back(fields(count - 1)[0], I(n_all - 1))
    for g in range(SLOTS):
        for s in range(NZ):
            @pl.when(goes_down(g) & (s >= z))
            def _():
                for ch in (s, TOP - s):
                    for d in zcopies(g, ch, -1, dsend):
                        d.wait_send()

            @pl.when((z < NZ - 1) & (s <= z))
            def _():
                for d in zcopies(g, s, 1, usend):
                    d.wait_send()
        for part in range(2):
            def keep():
                olocal(g, part).wait()
                for p in range(1, NX):
                    oremote(g, part, p, j, mod(j + p)).wait_send()
                    oremote(g, part, p, mod(j - p), j).wait_recv()

            def give():
                for p in range(NX):
                    oremote(g, part, p, mod(j - p), j).wait_recv()

            xpart(g, part, keep, give)

    @pl.when(z == 1)
    def _():
        for p in range(NX):
            oremote(1, 1, p, j, mod(j + p), shifted=True).wait_send()


def solution(mesh):
    assert mesh.shape["cx"] == NX and mesh.shape["cy"] == NZ
    spec = P(("batch", "cy", "cx"), None, None)

    def local(q, k, v):
        t, h, d = q.shape
        pc = t // 2
        rows = NX * pc
        c = d ** -0.5 * math.log2(math.e)
        tq = 2 * pc
        tiles = rows // tq
        f32, bf = jnp.float32, jnp.bfloat16
        dma = pltpu.SemaphoreType.DMA
        ot = pl.pallas_call(
            functools.partial(kernel, c),
            out_shape=jax.ShapeDtypeStruct((h, t, d), bf),
            in_specs=[pl.BlockSpec(memory_space=pl.ANY)] * 3,
            out_specs=pl.BlockSpec(memory_space=pl.ANY),
            scratch_shapes=[
                pltpu.VMEM((5, GQ, rows, d), bf),
                pltpu.VMEM((SLOTS, 2 * NZ, rows, d), bf),
                pltpu.VMEM((SLOTS, 2 * NZ, d, rows), bf),
                pltpu.VMEM((5, GQ * tiles, 1, tq), f32),
                pltpu.VMEM((5, GQ * tiles, 8, tq), f32),
                pltpu.VMEM((5, GQ * tiles, d, tq), f32),
                pltpu.VMEM((5, GQ, rows, d), bf),
                pltpu.VMEM((rows, tq), f32),
                pltpu.VMEM((rows, tq), f32),
                pltpu.VMEM((8, tq), f32),
                pltpu.VMEM((8, tq), f32),
                dma((SLOTS, 3, 2, NX)),
                dma((SLOTS, 3, 3, NX)),
                dma((SLOTS, 3, 2)),
                dma((SLOTS, 2 * NZ, 2)),
                dma((SLOTS, 2 * NZ, 2)),
                dma((SLOTS, 2 * NZ, 2)),
                dma((5, NX)),
                dma((4, NX)),
            ],
            compiler_params=pltpu.CompilerParams(
                collective_id=0, has_side_effects=True, vmem_limit_bytes=56 * 2**20),
        )(jnp.transpose(q, (1, 0, 2)), jnp.transpose(k, (1, 0, 2)), jnp.transpose(v, (1, 2, 0)))
        return jnp.transpose(ot, (1, 0, 2))

    return jax.shard_map(local, mesh=mesh, in_specs=(spec, spec, spec), out_specs=spec, check_vma=False)
```

```python
import functools
import math

import jax
import jax.numpy as jnp
from jax import lax
from jax.experimental import pallas as pl
from jax.experimental.pallas import tpu as pltpu
from jax.sharding import PartitionSpec as P


NX = 4
NZ = 4
SLOTS = 2
GQ = 3
NB = 4
NT = (((1,), (1,)), ((), ()))
MESH = pl.DeviceIdType.MESH
I = jnp.int32


def stage(c, nxt, cur):
    qn, kn_ref, s_nxt, x_nxt, base, rows = nxt
    tq = qn.shape[0]
    bk = kn_ref.shape[0] // NB
    blocks = rows // bk
    if cur is not None:
        s_cur, x_cur, v_ref, m_ref, l_ref, a_ref, keys = cur
        blocks = max(blocks, keys // bk)
        m0 = m_ref[...]
        m1 = jnp.maximum(m0, jnp.max(x_cur[...], axis=0, keepdims=True))
        al = jnp.exp2((m0 - m1) * c)
        m_ref[...] = m1
        lsum = l_ref[...] * al
    xm = o = None
    for b in range(blocks):
        r = slice(b * bk, (b + 1) * bk)
        if b * bk < rows:
            s = lax.dot_general(kn_ref[r, :], qn, NT, preferred_element_type=jnp.float32)
            if base is not None and (b + 1) * bk > base:
                kk = lax.broadcasted_iota(I, s.shape, 0) + b * bk
                qq = lax.broadcasted_iota(I, s.shape, 1) + base
                s = jnp.where(kk <= qq, s, -jnp.inf)
            s_nxt[r, :] = s
            y = jnp.max(s.reshape(bk // 8, 8, tq), axis=0)
            xm = y if xm is None else jnp.maximum(xm, y)
        if cur is not None and b * bk < keys:
            p = jnp.exp2((s_cur[r, :] - m1) * c)
            lsum = lsum + jnp.sum(p.reshape(bk // 8, 8, tq), axis=0)
            d = jnp.dot(v_ref[:, r], p.astype(jnp.bfloat16), preferred_element_type=jnp.float32)
            o = d if o is None else o + d
    x_nxt[...] = xm
    if cur is not None:
        l_ref[...] = lsum
        a_ref[...] = a_ref[...] * al + o


SHIFT = 4
TOP = 2 * NZ - 1
START, QUERY, EXTRA, BELOW, ABOVE = 1, 2, 3, 4, 5
RADIX = (5, 2, 8, 2, 6, 2, 2, 4)


def units(z):
    out = []

    def add(qs, ch, masked=0, act=0):
        out.append((qs, 1 if qs == SHIFT else qs // 2, ch, masked, act))

    def own(g, act):
        add(2 * g, z, 1, act)
        if not (g == 1 and z == 0):
            add(2 * g + 1, TOP - z, 1)
            add(2 * g + 1, z)

    own(0, START)
    for t in range(1, NZ):
        if z >= t:
            add(0, z - t, 0, BELOW)
            add(1, z - t)
        if z + t < NZ:
            add(1, z + t, 0, ABOVE)
            add(1, TOP - z - t, 0, ABOVE)
        if z == 0 and t == 1:
            own(1, QUERY)
    if z > 0:
        own(1, QUERY)
        add(SHIFT, z, 0, EXTRA)
        add(SHIFT, TOP - z)
        for t in range(1, NZ):
            if z >= t:
                add(SHIFT, z - t, 0, BELOW)
                add(2, z - t)
                add(3, z - t)
                add(SHIFT, TOP - z + t, int(z == t), BELOW)
            if z + t < NZ:
                for ch in (z + t, TOP - z - t):
                    add(SHIFT, ch, 0, ABOVE)
                    add(3, ch)
    last = {u[0]: i for i, u in enumerate(out)}
    return [u + (int(i == 3), int(last[u[0]] == i), 1 if u[0] == SHIFT else GQ) for i, u in enumerate(out)]


def pack(u):
    x = 0
    for r, f in zip(RADIX, u):
        x = x * r + f
    return x


def unpack(x):
    out = []
    for r in RADIX[::-1]:
        out.append(lax.rem(x, I(r)))
        x = lax.div(x, I(r))
    return out[::-1]


def kernel(c, q, k, v, o, qb, kb, vb, m, l, a, ost, sa, sb, xa, xb,
           xsend, xrecv, xloc, qsend, qrecv, zrecv, dsend, usend, osend, orecv):
    z = lax.axis_index("cy")
    j = lax.axis_index("cx")
    pc = k.shape[1] // 2
    tq = sa.shape[1]
    tiles = qb.shape[2] // tq

    def mod(x):
        return lax.rem(x + 2 * NX, I(NX))

    def chunk(part):
        return z if part == 0 else TOP - z

    def pos(part, jj):
        return jj if part == 0 else NX - 1 - jj

    def span(part, jj):
        return pl.ds(pl.multiple_of(pos(part, jj) * pc, pc), pc)

    barrier = pltpu.get_barrier_semaphore()
    for p in range(1, NX):
        pl.semaphore_signal(barrier, inc=1, device_id={"cx": mod(j + p)}, device_id_type=MESH)

    @pl.when(z > 1)
    def _():
        pl.semaphore_signal(barrier, inc=1, device_id={"cy": z - 1}, device_id_type=MESH)

    @pl.when((z > 0) & (z < NZ - 1))
    def _():
        pl.semaphore_signal(barrier, inc=1, device_id={"cy": z + 1}, device_id_type=MESH)

    for p in range(NX):
        @pl.when(z > 0)
        def _():
            pl.semaphore_signal(barrier, inc=1, device_id={"cy": I(0), "cx": mod(j + p)}, device_id_type=MESH)

        @pl.when(z == 0)
        def _():
            for zz in range(1, NZ):
                pl.semaphore_signal(barrier, inc=1, device_id={"cy": I(zz), "cx": mod(j + p)}, device_id_type=MESH)

    def by_z(values):
        x = I(values[-1])
        for zz in range(NZ - 1):
            x = jnp.where(z == zz, I(values[zz]), x)
        return x

    lists = [[pack(u) for u in units(zz)] for zz in range(NZ)]
    count = by_z([len(x) for x in lists])
    codes = [by_z([x[min(i, len(x) - 1)] for x in lists]) for i in range(max(map(len, lists)))]

    def fields(u):
        x = codes[-1]
        for i, code in enumerate(codes[:-1]):
            x = jnp.where(u == i, code, x)
        return unpack(x)

    pl.semaphore_wait(barrier, NX - 1 + by_z([NX * (NZ - 1)] + [NX + 2] * (NZ - 2) + [NX + 1]) - jnp.where(z == 1, 1, 0))

    def pair(g, kind, part, owner, dest):
        half = pl.ds(part * pc, pc)
        at = span(part, owner)
        if kind == 0:
            return k.at[SLOTS * dest + g, half, :], kb.at[g, chunk(part), at, :]
        if kind == 1:
            return v.at[SLOTS * dest + g, :, half], vb.at[g, chunk(part), :, at]
        return q.at[pl.ds(GQ * (SLOTS * dest + g), GQ), half, :], qb.at[2 * g + part, :, at, :]

    def xcopy(g, kind, part, p, owner, dest):
        src, dst = pair(g, kind, part, owner, dest)
        return pltpu.make_async_remote_copy(
            src_ref=src, dst_ref=dst, send_sem=xsend.at[g, kind, part, p - 1], recv_sem=xrecv.at[g, kind, part, p - 1],
            device_id={"cx": dest}, device_id_type=MESH)

    def xlocal(g, kind, part):
        src, dst = pair(g, kind, part, j, j)
        return pltpu.make_async_copy(src, dst, xloc.at[g, kind, part])

    for g in range(SLOTS):
        for kinds in ((0, 1), (2,)):
            for part in range(2):
                for p in range(1, NX):
                    for kind in kinds:
                        xcopy(g, kind, part, p, j, mod(j + p)).start()
                for kind in kinds:
                    xlocal(g, kind, part).start()

    def xwait(g, kinds):
        for part in range(2):
            for kind in kinds:
                xlocal(g, kind, part).wait()
                for p in range(1, NX):
                    xcopy(g, kind, part, p, mod(j - p), j).wait_recv()

    def shift(zz):
        return pltpu.make_async_remote_copy(
            src_ref=qb.at[3, zz - 1], dst_ref=qb.at[SHIFT, 0], send_sem=qsend.at[zz - 1], recv_sem=qrecv.at[0],
            device_id={"cy": I(zz)}, device_id_type=MESH)

    def zcopies(g, ch, dz, send):
        return [
            pltpu.make_async_remote_copy(
                src_ref=buf.at[g, ch], dst_ref=buf.at[g, ch], send_sem=send.at[g, ch, i], recv_sem=zrecv.at[g, ch, i],
                device_id={"cy": z + dz}, device_id_type=MESH)
            for i, buf in enumerate((kb, vb))
        ]

    def goes_down(g):
        return z > jnp.where(g == 1, 1, 0)

    def down(g, ch):
        @pl.when(goes_down(g))
        def _():
            for d in zcopies(g, ch, -1, dsend):
                d.start()

    def up(g, ch):
        @pl.when(z < NZ - 1)
        def _():
            for d in zcopies(g, ch, 1, usend):
                d.start()

    m[...] = jnp.full_like(m, -jnp.inf)
    l[...] = jnp.zeros_like(l)

    @pl.loop(0, 5)
    def _(i):
        a[i] = jnp.zeros(a.shape[1:], a.dtype)

    def before(f):
        _, g, ch, _, act, kv, _, _ = f

        def begin(g):
            xwait(g, (0, 1))
            for ch in (z, TOP - z):
                down(I(g), ch)
            up(I(g), z)
            if g == 1:
                up(I(g), TOP - z)

        pl.when(kv == 1)(lambda: begin(1))

        @pl.when(act == START)
        def _():
            begin(0)
            xwait(0, (2,))

        @pl.when(act == QUERY)
        def _():
            xwait(1, (2,))

            @pl.when(z == 0)
            def _():
                for zz in range(1, NZ):
                    shift(zz).start()

        @pl.when(act == EXTRA)
        def _():
            shift(1).wait_recv()

        @pl.when(act == BELOW)
        def _():
            for d in zcopies(g, ch, 1, usend):
                d.wait_recv()
            up(g, ch)

        @pl.when(act == ABOVE)
        def _():
            for d in zcopies(g, ch, -1, dsend):
                d.wait_recv()
            down(g, ch)

    def opiece(g, part, owner, dest, heads, hd, shifted):
        qs, to = (SHIFT, hd + z - 1) if shifted else (2 * g + part, hd)
        return dict(
            src_ref=ost.at[qs, pl.ds(hd, heads), span(part, dest), :],
            dst_ref=o.at[pl.ds(GQ * (SLOTS * owner + g) + to, heads), pl.ds(part * pc, pc), :])

    def oremote(g, part, p, owner, dest, heads=GQ, hd=0, shifted=False):
        return pltpu.make_async_remote_copy(
            **opiece(g, part, owner, dest, heads, hd, shifted),
            send_sem=osend.at[SHIFT if shifted else 2 * g + part, p], recv_sem=orecv.at[2 * g + part, p],
            device_id={"cy": I(0) if shifted else z, "cx": dest}, device_id_type=MESH)

    def olocal(g, part, heads=GQ, hd=0):
        r = opiece(g, part, j, j, heads, hd, False)
        return pltpu.make_async_copy(r["src_ref"], r["dst_ref"], osend.at[2 * g + part, 0])

    def finish(qs, n):
        y = a[qs, n] / jnp.sum(l[qs, n], axis=0, keepdims=True)
        at = pl.ds(pl.multiple_of(lax.rem(n, I(tiles)) * tq, tq), tq)
        ost[qs, lax.div(n, I(tiles)), at, :] = y.astype(ost.dtype).T

    def give_back(qs, n):
        hd = lax.div(n, I(tiles))
        for case in range(5):
            @pl.when(qs == case)
            def _():
                shifted = case == SHIFT
                g, part = (1, 1) if shifted else (case // 2, case % 2)
                for e in range(tq // pc):
                    at = lax.rem(n, I(tiles)) * (tq // pc) + e
                    dest = pos(part, at)
                    p = mod(dest - j)
                    if shifted:
                        oremote(g, part, p, j, dest, 1, hd, True).start()
                    else:
                        pl.when(p == 0)(lambda: olocal(g, part, 1, hd).start())
                        pl.when(p > 0)(lambda: oremote(g, part, p, j, dest, 1, hd).start())

    def after(f, n, w, nw):
        pl.when(f[6] == 1)(lambda: finish(f[0], n))
        pl.when(w[6] == 1)(lambda: give_back(w[0], nw))

    def nxt(f, n, s, x, odd, masked):
        at = pl.ds(odd * tq, tq)
        rows = kb.shape[2] if odd or not masked else tq
        return (qb[f[0], lax.div(I(n), I(tiles)), at, :], kb.at[f[1], f[2]], s, x, odd * tq if masked else None, rows)

    def step(fn, nn, s_n, x_n, f, n, s_c, x_c, odd):
        qs = f[0]
        for masked in (False, True):
            @pl.when(fn[3] == int(masked))
            def _():
                keys = tq if odd and masked else kb.shape[2]
                stage(c, nxt(fn, nn, s_n, x_n, odd, masked),
                      (s_c, x_c, vb.at[f[1], f[2]], m.at[qs, n], l.at[qs, n], a.at[qs, n], keys))

    first = fields(I(0))
    before(first)
    stage(c, nxt(first, 0, sa, xa, 0, True), None)

    @pl.loop(0, count)
    def _(u):
        f = fields(u)
        fn = fields(jnp.minimum(u + 1, count - 1))
        w = fields(jnp.maximum(u - 1, 0))
        w[6] = jnp.where(u > 0, w[6], 0)

        @pl.loop(0, f[7])
        def _(i):
            n = tiles * i
            step(f, n + 1, sb, xb, f, n, sa, xa, 1)
            after(f, n, [jnp.where(i == 0, p, q) for p, q in zip(w, f)], jnp.where(i == 0, tiles * w[7] - 1, n - 1))
            wrap = i == f[7] - 1
            pl.when(wrap & (u + 1 < count))(lambda: before(fn))
            step([jnp.where(wrap, p, q) for p, q in zip(fn, f)], jnp.where(wrap, 0, n + 2), sa, xa, f, n + 1, sb, xb, 0)
            after(f, n + 1, f, n)

    for g in range(SLOTS):
        for part in range(2):
            for p in range(1, NX):
                for kind in range(3):
                    xcopy(g, kind, part, p, j, mod(j + p)).wait_send()
    end = fields(count - 1)
    give_back(end[0], tiles * end[7] - 1)
    for g in range(SLOTS):
        for s in range(NZ):
            @pl.when(goes_down(g) & (s >= z))
            def _():
                for ch in (s, TOP - s):
                    for d in zcopies(g, ch, -1, dsend):
                        d.wait_send()

            @pl.when((z < NZ - 1) & (s <= z))
            def _():
                for ch in (s,) if g == 0 else (s, TOP - s):
                    for d in zcopies(g, ch, 1, usend):
                        d.wait_send()
        for part in range(2):
            def keep():
                olocal(g, part).wait()
                for p in range(1, NX):
                    oremote(g, part, p, j, mod(j + p)).wait_send()
                    oremote(g, part, p, mod(j - p), j).wait_recv()

            def given():
                for p in range(NX):
                    oremote(g, part, p, mod(j - p), j).wait_recv()

            if g == 1 and part == 1:
                pl.when(z == 0)(given)
                pl.when(z > 0)(keep)
            else:
                keep()

    @pl.when(z == 0)
    def _():
        for zz in range(1, NZ):
            shift(zz).wait_send()

    @pl.when(z > 0)
    def _():
        for p in range(NX):
            oremote(1, 1, p, j, mod(j + p), 1, shifted=True).wait_send()


def solution(mesh):
    assert mesh.shape["cx"] == NX and mesh.shape["cy"] == NZ
    spec = P(("batch", "cy", "cx"), None, None)

    def local(q, k, v):
        t, h, d = q.shape
        pc = t // 2
        rows = NX * pc
        c = d ** -0.5 * math.log2(math.e)
        tq = 2 * pc
        tiles = rows // tq
        f32, bf = jnp.float32, jnp.bfloat16
        dma = pltpu.SemaphoreType.DMA
        ot = pl.pallas_call(
            functools.partial(kernel, c),
            out_shape=jax.ShapeDtypeStruct((h, t, d), bf),
            in_specs=[pl.BlockSpec(memory_space=pl.ANY)] * 3,
            out_specs=pl.BlockSpec(memory_space=pl.ANY),
            scratch_shapes=[
                pltpu.VMEM((5, GQ, rows, d), bf),
                pltpu.VMEM((SLOTS, 2 * NZ, rows, d), bf),
                pltpu.VMEM((SLOTS, 2 * NZ, d, rows), bf),
                pltpu.VMEM((5, GQ * tiles, 1, tq), f32),
                pltpu.VMEM((5, GQ * tiles, 8, tq), f32),
                pltpu.VMEM((5, GQ * tiles, d, tq), f32),
                pltpu.VMEM((5, GQ, rows, d), bf),
                pltpu.VMEM((rows, tq), f32),
                pltpu.VMEM((rows, tq), f32),
                pltpu.VMEM((8, tq), f32),
                pltpu.VMEM((8, tq), f32),
                dma((SLOTS, 3, 2, NX - 1)),
                dma((SLOTS, 3, 2, NX - 1)),
                dma((SLOTS, 3, 2)),
                dma((NZ - 1,)),
                dma((1,)),
                dma((SLOTS, 2 * NZ, 2)),
                dma((SLOTS, 2 * NZ, 2)),
                dma((SLOTS, 2 * NZ, 2)),
                dma((5, NX)),
                dma((4, NX)),
            ],
            compiler_params=pltpu.CompilerParams(
                collective_id=0, has_side_effects=True, vmem_limit_bytes=56 * 2**20),
        )(jnp.transpose(q, (1, 0, 2)), jnp.transpose(k, (1, 0, 2)), jnp.transpose(v, (1, 2, 0)))
        return jnp.transpose(ot, (1, 0, 2))

    return jax.shard_map(local, mesh=mesh, in_specs=(spec, spec, spec), out_specs=spec, check_vma=False)
```

```python
import functools
import math

import jax
import jax.numpy as jnp
from jax import lax
from jax.experimental import pallas as pl
from jax.experimental.pallas import tpu as pltpu
from jax.sharding import PartitionSpec as P


NX = 4
NZ = 4
SLOTS = 2
GQ = 3
NB = 4
NT = (((1,), (1,)), ((), ()))
MESH = pl.DeviceIdType.MESH
I = jnp.int32


def stage(c, nxt, cur):
    qn, kn_ref, s_nxt, x_nxt, base, rows = nxt
    tq = qn.shape[0]
    bk = kn_ref.shape[0] // NB
    blocks = rows // bk
    if cur is not None:
        s_cur, x_cur, v_ref, m_ref, l_ref, a_ref, keys = cur
        blocks = max(blocks, keys // bk)
        m0 = m_ref[...]
        m1 = jnp.maximum(m0, jnp.max(x_cur[...], axis=0, keepdims=True))
        al = jnp.exp2((m0 - m1) * c)
        m_ref[...] = m1
        lsum = l_ref[...] * al
    xm = o = None
    for b in range(blocks):
        r = slice(b * bk, (b + 1) * bk)
        if b * bk < rows:
            s = lax.dot_general(kn_ref[r, :], qn, NT, preferred_element_type=jnp.float32)
            if base is not None and (b + 1) * bk > base:
                kk = lax.broadcasted_iota(I, s.shape, 0) + b * bk
                qq = lax.broadcasted_iota(I, s.shape, 1) + base
                s = jnp.where(kk <= qq, s, -jnp.inf)
            s_nxt[r, :] = s
            y = jnp.max(s.reshape(bk // 8, 8, tq), axis=0)
            xm = y if xm is None else jnp.maximum(xm, y)
        if cur is not None and b * bk < keys:
            p = jnp.exp2((s_cur[r, :] - m1) * c)
            lsum = lsum + jnp.sum(p.reshape(bk // 8, 8, tq), axis=0)
            d = jnp.dot(v_ref[:, r], p.astype(jnp.bfloat16), preferred_element_type=jnp.float32)
            o = d if o is None else o + d
    x_nxt[...] = xm
    if cur is not None:
        l_ref[...] = lsum
        a_ref[...] = a_ref[...] * al + o


SHIFT = 4
SHARE = {1: (0, 2), 2: (2, 1)}
FAR = max(SHARE)
TOP = 2 * NZ - 1
KV1, QUERY, EXTRA, LAND = 1, 2, 3, 4
RADIX = (5, 2, 8, 2, 2, 4, 2, 20, 20, 20)

ORDER = (
    ((0, 0, 5), (1, 7), (1, 0), (1, 1, 10), (1, 6, 1), (1, 2, 6), (2, 0, 2), (1, 5, 9), (1, 3, 7), (1, 4, 8)),
    ((0, 1, 4, 6), (0, 0), (1, 6, 9), (1, 0), (1, 1, 1), (1, 2), (1, 3, 7), (1, 5), (1, 4, 12, 2, 8), (2, 1), (2, 0),
     (3, 6, 19), (3, 0, 14), (3, 1), (4, 7, 3), (4, 0, 17), (4, 1), (4, 2), (4, 5), (4, 3, 15), (4, 6), (3, 2), (3, 3),
     (4, 4, 16), (3, 4), (3, 5)),
    ((0, 2, 5, 7), (0, 1), (1, 5, 8), (1, 1), (0, 0, 1, 4), (1, 0), (1, 2), (1, 3), (1, 4, 13, 15, 2), (2, 2), (2, 1),
     (3, 5, 16, 18), (3, 1), (3, 2), (3, 3), (3, 4), (4, 1, 3), (4, 2), (4, 3), (4, 4), (4, 5), (4, 6), (4, 0, 12), (2, 0),
     (3, 0), (4, 7, 19)),
    ((0, 3, 6), (0, 2), (1, 4), (1, 2), (0, 1, 1, 5), (1, 1), (1, 3), (2, 3, 14, 2), (2, 2), (3, 4), (0, 0, 4), (1, 0), (3, 2),
     (2, 1, 13), (3, 1), (3, 3), (2, 0, 12), (3, 0)),
)

def units(z):
    out = []
    steps = 0
    work = ORDER[z]
    last = {u[0]: i for i, u in enumerate(work)}
    for i, (qs, ch, *acts) in enumerate(work):
        heads = SHARE[z][1] if qs == SHIFT else GQ
        diagonal = TOP if qs == SHIFT else z if qs % 2 == 0 else TOP - z
        out.append((qs, 1 if qs == SHIFT else qs // 2, ch, int(ch == diagonal), int(last[qs] == i), heads, steps % 2,
                    *acts, *[0] * (3 - len(acts))))
        steps += heads
    return out


def pack(u):
    x = 0
    for r, f in zip(RADIX, u):
        x = x * r + f
    return x


def unpack(x):
    out = []
    for r in RADIX[::-1]:
        out.append(lax.rem(x, I(r)))
        x = lax.div(x, I(r))
    return out[::-1]


def kernel(c, q, k, v, o, qb, kb, vb, m, l, a, ost, sa, sb, xa, xb,
           xsend, xrecv, xloc, qsend, qrecv, zrecv, dsend, usend, osend, orecv):
    z = lax.axis_index("cy")
    j = lax.axis_index("cx")
    pc = k.shape[1] // 2
    tq = sa.shape[2]
    tiles = qb.shape[2] // tq

    def mod(x):
        return lax.rem(x + 2 * NX, I(NX))

    def chunk(part):
        return z if part == 0 else TOP - z

    def pos(part, jj):
        return jj if part == 0 else NX - 1 - jj

    def span(part, jj):
        return pl.ds(pl.multiple_of(pos(part, jj) * pc, pc), pc)

    barrier = pltpu.get_barrier_semaphore()
    for p in range(1, NX):
        pl.semaphore_signal(barrier, inc=1, device_id={"cx": mod(j + p)}, device_id_type=MESH)

    @pl.when(z > 1)
    def _():
        pl.semaphore_signal(barrier, inc=1, device_id={"cy": z - 1}, device_id_type=MESH)

    @pl.when((z > 0) & (z < NZ - 1))
    def _():
        pl.semaphore_signal(barrier, inc=1, device_id={"cy": z + 1}, device_id_type=MESH)

    for p in range(NX):
        @pl.when((z > 0) & (z <= FAR))
        def _():
            pl.semaphore_signal(barrier, inc=1, device_id={"cy": I(0), "cx": mod(j + p)}, device_id_type=MESH)

        @pl.when(z == 0)
        def _():
            for zz in SHARE:
                pl.semaphore_signal(barrier, inc=1, device_id={"cy": I(zz), "cx": mod(j + p)}, device_id_type=MESH)

    def by_z(values):
        x = I(values[-1])
        for zz in range(NZ - 1):
            x = jnp.where(z == zz, I(values[zz]), x)
        return x

    lists = [[pack(u) for u in units(zz)] for zz in range(NZ)]
    count = by_z([len(x) for x in lists])
    codes = [by_z([x[min(i, len(x) - 1)] for x in lists]) for i in range(max(map(len, lists)))]

    def fields(u):
        x = codes[-1]
        for i, code in enumerate(codes[:-1]):
            x = jnp.where(u == i, code, x)
        return unpack(x)

    pl.semaphore_wait(barrier, NX - 1 + by_z([NX * FAR, NX + 1, NX + 2, 1]))

    def pair(g, kind, part, owner, dest):
        half = pl.ds(part * pc, pc)
        at = span(part, owner)
        if kind == 0:
            return k.at[SLOTS * dest + g, half, :], kb.at[g, chunk(part), at, :]
        if kind == 1:
            return v.at[SLOTS * dest + g, :, half], vb.at[g, chunk(part), :, at]
        return q.at[pl.ds(GQ * (SLOTS * dest + g), GQ), half, :], qb.at[2 * g + part, :, at, :]

    def xcopy(g, kind, part, p, owner, dest):
        src, dst = pair(g, kind, part, owner, dest)
        return pltpu.make_async_remote_copy(
            src_ref=src, dst_ref=dst, send_sem=xsend.at[g, kind, part, p - 1], recv_sem=xrecv.at[g, kind, part, p - 1],
            device_id={"cx": dest}, device_id_type=MESH)

    def xlocal(g, kind, part):
        src, dst = pair(g, kind, part, j, j)
        return pltpu.make_async_copy(src, dst, xloc.at[g, kind, part])

    for g in range(SLOTS):
        for kinds in ((0, 1), (2,)):
            for part in range(2):
                for p in range(1, NX):
                    for kind in kinds:
                        xcopy(g, kind, part, p, j, mod(j + p)).start()
                for kind in kinds:
                    xlocal(g, kind, part).start()

    def xwait(g, kinds):
        for part in range(2):
            for kind in kinds:
                xlocal(g, kind, part).wait()
                for p in range(1, NX):
                    xcopy(g, kind, part, p, mod(j - p), j).wait_recv()

    def shift(zz):
        return pltpu.make_async_remote_copy(
            src_ref=qb.at[3, pl.ds(*SHARE[zz])], dst_ref=qb.at[SHIFT, pl.ds(0, SHARE[zz][1])], send_sem=qsend.at[zz - 1], recv_sem=qrecv.at[0],
            device_id={"cy": I(zz)}, device_id_type=MESH)

    def zcopies(g, ch, dz, send):
        return [
            pltpu.make_async_remote_copy(
                src_ref=buf.at[g, ch], dst_ref=buf.at[g, ch], send_sem=send.at[g, ch, i], recv_sem=zrecv.at[g, ch, i],
                device_id={"cy": z + dz}, device_id_type=MESH)
            for i, buf in enumerate((kb, vb))
        ]

    def goes_down(g):
        return z > jnp.where(g == 1, 1, 0)

    def down(g, ch):
        @pl.when(goes_down(g))
        def _():
            for d in zcopies(g, ch, -1, dsend):
                d.start()

    def up(g, ch):
        @pl.when(z < jnp.where(ch < NZ, NZ - 1, FAR))
        def _():
            for d in zcopies(g, ch, 1, usend):
                d.start()

    m[...] = jnp.full_like(m, -jnp.inf)
    l[...] = jnp.zeros_like(l)

    @pl.loop(0, 5)
    def _(i):
        a[i] = jnp.zeros(a.shape[1:], a.dtype)

    def begin(g):
        xwait(g, (0, 1))
        for ch in (z, TOP - z):
            down(I(g), ch)
        up(I(g), z)
        if g == 1:
            up(I(g), TOP - z)

    def before(f):
        @pl.loop(0, 3)
        def _(i):
            act = jnp.where(i == 0, f[7], jnp.where(i == 1, f[8], f[9]))
            pl.when(act == KV1)(lambda: begin(1))

            @pl.when(act == QUERY)
            def _():
                xwait(1, (2,))

                @pl.when(z == 0)
                def _():
                    for zz in SHARE:
                        shift(zz).start()

            @pl.when(act == EXTRA)
            def _():
                for zz in SHARE:
                    pl.when(z == zz)(lambda: shift(zz).wait_recv())

            @pl.when(act >= LAND)
            def _():
                g = lax.div(act - LAND, I(2 * NZ))
                ch = lax.rem(jnp.maximum(act - LAND, 0), I(2 * NZ))
                source = jnp.where(ch < NZ, ch, TOP - ch)

                @pl.when(source < z)
                def _():
                    for d in zcopies(g, ch, 1, usend):
                        d.wait_recv()
                    up(g, ch)

                @pl.when(source > z)
                def _():
                    for d in zcopies(g, ch, -1, dsend):
                        d.wait_recv()
                    down(g, ch)

    def opiece(g, part, owner, dest, heads, hd, shifted):
        qs, to = (SHIFT, hd + 2 * (z - 1)) if shifted else (2 * g + part, hd)
        return dict(
            src_ref=ost.at[qs, pl.ds(hd, heads), span(part, dest), :],
            dst_ref=o.at[pl.ds(GQ * (SLOTS * owner + g) + to, heads), pl.ds(part * pc, pc), :])

    def oremote(g, part, p, owner, dest, heads=GQ, hd=0, shifted=False):
        return pltpu.make_async_remote_copy(
            **opiece(g, part, owner, dest, heads, hd, shifted),
            send_sem=osend.at[SHIFT if shifted else 2 * g + part, p], recv_sem=orecv.at[2 * g + part, p],
            device_id={"cy": I(0) if shifted else z, "cx": dest}, device_id_type=MESH)

    def olocal(g, part, heads=GQ, hd=0):
        r = opiece(g, part, j, j, heads, hd, False)
        return pltpu.make_async_copy(r["src_ref"], r["dst_ref"], osend.at[2 * g + part, 0])

    def finish(qs, n):
        y = a[qs, n] / jnp.sum(l[qs, n], axis=0, keepdims=True)
        at = pl.ds(pl.multiple_of(lax.rem(n, I(tiles)) * tq, tq), tq)
        ost[qs, lax.div(n, I(tiles)), at, :] = y.astype(ost.dtype).T

    def give_back(qs, n):
        hd = lax.div(n, I(tiles))
        for case in range(5):
            @pl.when(qs == case)
            def _():
                shifted = case == SHIFT
                g, part = (1, 1) if shifted else (case // 2, case % 2)
                for e in range(tq // pc):
                    at = lax.rem(n, I(tiles)) * (tq // pc) + e
                    dest = pos(part, at)
                    p = mod(dest - j)
                    if shifted:
                        oremote(g, part, p, j, dest, 1, hd, True).start()
                    else:
                        pl.when(p == 0)(lambda: olocal(g, part, 1, hd).start())
                        pl.when(p > 0)(lambda: oremote(g, part, p, j, dest, 1, hd).start())

    def after(f, h, w, hw):
        @pl.when(f[4] == 1)
        def _():
            for e in range(tiles):
                finish(f[0], tiles * h + e)

        @pl.when(w[4] == 1)
        def _():
            for e in range(tiles):
                give_back(w[0], tiles * hw + e)

    bufs = ((sa, xa), (sb, xb))

    def nxt(f, h, e, par, masked):
        rows = (e + 1) * tq if masked else kb.shape[2]
        sx, xx = bufs[par]
        return qb[f[0], h, pl.ds(e * tq, tq), :], kb.at[f[1], f[2]], sx.at[e], xx.at[e], e * tq if masked else None, rows

    def step(fn, hn, f, h):
        qs = f[0]
        parity = lax.rem(f[6] + h, I(2))
        for par in range(2):
            for m_cur in (False, True):
                for m_nxt in (False, True):
                    @pl.when((parity == par) & (f[3] == int(m_cur)) & (fn[3] == int(m_nxt)))
                    def _():
                        for e in range(tiles):
                            n = tiles * h + e
                            sx, xx = bufs[par]
                            keys = (e + 1) * tq if m_cur else kb.shape[2]
                            stage(c, nxt(fn, hn, e, 1 - par, m_nxt),
                                  (sx.at[e], xx.at[e], vb.at[f[1], f[2]], m.at[qs, n], l.at[qs, n], a.at[qs, n], keys))

    first = fields(I(0))
    begin(0)
    xwait(0, (2,))
    before(first)
    for e in range(tiles):
        stage(c, nxt(first, 0, e, 0, True), None)

    @pl.loop(0, count)
    def _(u):
        f = fields(u)
        fn = fields(jnp.minimum(u + 1, count - 1))
        w = fields(jnp.maximum(u - 1, 0))
        w[4] = jnp.where(u > 0, w[4], 0)

        @pl.loop(0, f[5])
        def _(h):
            wrap = h == f[5] - 1
            pl.when(wrap & (u + 1 < count))(lambda: before(fn))
            step([jnp.where(wrap, p, q) for p, q in zip(fn, f)], jnp.where(wrap, 0, h + 1), f, h)
            after(f, h, [jnp.where(h == 0, p, q) for p, q in zip(w, f)], jnp.where(h == 0, w[5] - 1, h - 1))

    for g in range(SLOTS):
        for part in range(2):
            for p in range(1, NX):
                for kind in range(3):
                    xcopy(g, kind, part, p, j, mod(j + p)).wait_send()
    end = fields(count - 1)
    for e in range(tiles):
        give_back(end[0], tiles * (end[5] - 1) + e)
    for g in range(SLOTS):
        for s in range(NZ):
            @pl.when(goes_down(g) & (s >= z))
            def _():
                for ch in (s, TOP - s):
                    for d in zcopies(g, ch, -1, dsend):
                        d.wait_send()

            @pl.when((z < NZ - 1) & (s <= z))
            def _():
                for d in zcopies(g, s, 1, usend):
                    d.wait_send()

            if g == 1:
                @pl.when((z < FAR) & (s <= z))
                def _():
                    for d in zcopies(g, TOP - s, 1, usend):
                        d.wait_send()
        for part in range(2):
            def keep():
                olocal(g, part).wait()
                for p in range(1, NX):
                    oremote(g, part, p, j, mod(j + p)).wait_send()
                    oremote(g, part, p, mod(j - p), j).wait_recv()

            def given():
                for p in range(NX):
                    oremote(g, part, p, mod(j - p), j).wait_recv()

            if g == 1 and part == 1:
                pl.when(z == 0)(given)
                pl.when(z > 0)(keep)
            else:
                keep()

    @pl.when(z == 0)
    def _():
        for zz in SHARE:
            shift(zz).wait_send()

    for zz in SHARE:
        @pl.when(z == zz)
        def _():
            for p in range(NX):
                oremote(1, 1, p, j, mod(j + p), SHARE[zz][1], shifted=True).wait_send()


def solution(mesh):
    assert mesh.shape["cx"] == NX and mesh.shape["cy"] == NZ
    spec = P(("batch", "cy", "cx"), None, None)

    def local(q, k, v):
        t, h, d = q.shape
        pc = t // 2
        rows = NX * pc
        c = d ** -0.5 * math.log2(math.e)
        tq = 2 * pc
        tiles = rows // tq
        f32, bf = jnp.float32, jnp.bfloat16
        dma = pltpu.SemaphoreType.DMA
        ot = pl.pallas_call(
            functools.partial(kernel, c),
            out_shape=jax.ShapeDtypeStruct((h, t, d), bf),
            in_specs=[pl.BlockSpec(memory_space=pl.ANY)] * 3,
            out_specs=pl.BlockSpec(memory_space=pl.ANY),
            scratch_shapes=[
                pltpu.VMEM((5, GQ, rows, d), bf),
                pltpu.VMEM((SLOTS, 2 * NZ, rows, d), bf),
                pltpu.VMEM((SLOTS, 2 * NZ, d, rows), bf),
                pltpu.VMEM((5, GQ * tiles, 1, tq), f32),
                pltpu.VMEM((5, GQ * tiles, 8, tq), f32),
                pltpu.VMEM((5, GQ * tiles, d, tq), f32),
                pltpu.VMEM((5, GQ, rows, d), bf),
                pltpu.VMEM((tiles, rows, tq), f32),
                pltpu.VMEM((tiles, rows, tq), f32),
                pltpu.VMEM((tiles, 8, tq), f32),
                pltpu.VMEM((tiles, 8, tq), f32),
                dma((SLOTS, 3, 2, NX - 1)),
                dma((SLOTS, 3, 2, NX - 1)),
                dma((SLOTS, 3, 2)),
                dma((NZ - 1,)),
                dma((1,)),
                dma((SLOTS, 2 * NZ, 2)),
                dma((SLOTS, 2 * NZ, 2)),
                dma((SLOTS, 2 * NZ, 2)),
                dma((5, NX)),
                dma((4, NX)),
            ],
            compiler_params=pltpu.CompilerParams(
                collective_id=0, has_side_effects=True, vmem_limit_bytes=56 * 2**20),
        )(jnp.transpose(q, (1, 0, 2)), jnp.transpose(k, (1, 0, 2)), jnp.transpose(v, (1, 2, 0)))
        return jnp.transpose(ot, (1, 0, 2))

    return jax.shard_map(local, mesh=mesh, in_specs=(spec, spec, spec), out_specs=spec, check_vma=False)
```

```python
import functools
import math

import jax
import jax.numpy as jnp
from jax import lax
from jax.experimental import pallas as pl
from jax.experimental.pallas import tpu as pltpu
from jax.sharding import PartitionSpec as P


NX = 4
NZ = 4
SLOTS = 2
GQ = 3
NB = 4
NT = (((1,), (1,)), ((), ()))
MESH = pl.DeviceIdType.MESH
I = jnp.int32


def stage(c, nxt, cur):
    qn, kn_ref, s_nxt, x_nxt, base, rows = nxt
    tq = qn.shape[0]
    bk = kn_ref.shape[0] // NB
    blocks = rows // bk
    if cur is not None:
        s_cur, x_cur, v_ref, m_ref, l_ref, a_ref, keys = cur
        blocks = max(blocks, keys // bk)
        m0 = m_ref[...]
        m1 = jnp.maximum(m0, jnp.max(x_cur[...], axis=0, keepdims=True))
        al = jnp.exp2((m0 - m1) * c)
        m_ref[...] = m1
        lsum = l_ref[...] * al
    xm = o = None
    for b in range(blocks):
        r = slice(b * bk, (b + 1) * bk)
        if b * bk < rows:
            s = lax.dot_general(kn_ref[r, :], qn, NT, preferred_element_type=jnp.float32)
            if base is not None and (b + 1) * bk > base:
                kk = lax.broadcasted_iota(I, s.shape, 0) + b * bk
                qq = lax.broadcasted_iota(I, s.shape, 1) + base
                s = jnp.where(kk <= qq, s, -jnp.inf)
            s_nxt[r, :] = s
            y = jnp.max(s.reshape(bk // 8, 8, tq), axis=0)
            xm = y if xm is None else jnp.maximum(xm, y)
        if cur is not None and b * bk < keys:
            p = jnp.exp2((s_cur[r, :] - m1) * c)
            lsum = lsum + jnp.sum(p.reshape(bk // 8, 8, tq), axis=0)
            d = jnp.dot(v_ref[:, r], p.astype(jnp.bfloat16), preferred_element_type=jnp.float32)
            o = d if o is None else o + d
    x_nxt[...] = xm
    if cur is not None:
        l_ref[...] = lsum
        a_ref[...] = a_ref[...] * al + o


SHIFT = 4
SHARE = {1: (0, 2), 2: (2, 1)}
FAR = max(SHARE)
TOP = 2 * NZ - 1
KV1, QUERY, EXTRA, LAND, HIGH = 1, 2, 3, 4, 20
RADIX = (5, 2, 8, 2, 2, 4, 2, 21, 21, 21, 3)

ORDER = (
    ((0, 0), (1, 7, 5, 20), (1, 0), (1, 1, 10), (1, 6), (1, 2, 1, 6), (2, 0, 2), (1, 5, 9), (1, 3, 7), (1, 4, 8)),
    ((0, 1), (0, 0, 4, 6), (1, 6, 20), (1, 0), (1, 1, 9), (1, 2), (1, 5, 1), (1, 3, 7), (2, 1, 12, 2), (1, 4, 8), (2, 0),
     (3, 6, 19), (3, 0, 14), (3, 1), (3, 2), (4, 7, 3, 17), (4, 0), (4, 1), (4, 2), (4, 3, 15), (4, 5), (4, 6), (3, 3),
     (4, 4, 16), (3, 4), (3, 5)),
    ((0, 2), (0, 1, 5, 7), (1, 5, 20), (1, 1), (1, 2, 8), (0, 0, 4), (1, 0, 1), (1, 3), (1, 4), (2, 2, 13, 15, 2), (2, 1),
     (3, 5), (3, 1), (2, 0, 16, 12), (3, 0), (3, 2), (3, 3, 18), (3, 4), (4, 7, 19, 3), (4, 0), (4, 1), (4, 2), (4, 3), (4, 4),
     (4, 5), (4, 6)),
    ((0, 3), (0, 2, 6), (1, 4, 20), (1, 2), (1, 3), (0, 1, 5), (1, 1, 1), (0, 0, 4), (1, 0), (2, 3, 2), (3, 4), (2, 2, 14),
     (3, 2), (3, 3), (2, 1, 13), (3, 1), (2, 0, 12), (3, 0)),
)


def units(z):
    work = list(ORDER[z])
    if z > 0:
        k = len(work)
        while work[k - 1][0] == 3 and len(work[k - 1]) == 2 and len(work) - k < 3:
            k -= 1
        work = [(w, 0, SHARE[z][1] if w[0] == SHIFT else GQ) for w in work[:k]] + [
            (w, h, 1) for h in range(GQ) for w in work[k:]]
    else:
        work = [(w, 0, GQ) for w in work]
    last = {(w[0], h): i for i, (w, h0, n) in enumerate(work) for h in range(h0, h0 + n)}
    out = []
    steps = 0
    for i, ((qs, ch, *acts), h0, heads) in enumerate(work):
        diagonal = TOP if qs == SHIFT else z if qs % 2 == 0 else TOP - z
        ends = [last[qs, h] == i for h in range(h0, h0 + heads)]
        assert all(ends) or not any(ends)
        out.append((qs, 1 if qs == SHIFT else qs // 2, ch, int(ch == diagonal), int(ends[0]), heads, steps % 2,
                    *acts, *[0] * (3 - len(acts)), h0))
        steps += heads
    return out


def pack(u):
    x = 0
    for r, f in zip(RADIX, u):
        x = x * r + f
    return x


def unpack(x):
    out = []
    for r in RADIX[::-1]:
        out.append(lax.rem(x, I(r)))
        x = lax.div(x, I(r))
    return out[::-1]


def kernel(c, q, k, v, o, qb, kb, vb, m, l, a, ost, sa, sb, xa, xb,
           xsend, xrecv, xloc, qsend, qrecv, zrecv, dsend, usend, osend, orecv):
    z = lax.axis_index("cy")
    j = lax.axis_index("cx")
    pc = k.shape[1] // 2
    tq = sa.shape[2]
    tiles = qb.shape[2] // tq

    def mod(x):
        return lax.rem(x + 2 * NX, I(NX))

    def chunk(part):
        return z if part == 0 else TOP - z

    def pos(part, jj):
        return jj if part == 0 else NX - 1 - jj

    def span(part, jj):
        return pl.ds(pl.multiple_of(pos(part, jj) * pc, pc), pc)

    barrier = pltpu.get_barrier_semaphore()
    for p in range(1, NX):
        pl.semaphore_signal(barrier, inc=1, device_id={"cx": mod(j + p)}, device_id_type=MESH)

    @pl.when(z > 1)
    def _():
        pl.semaphore_signal(barrier, inc=1, device_id={"cy": z - 1}, device_id_type=MESH)

    @pl.when((z > 0) & (z < NZ - 1))
    def _():
        pl.semaphore_signal(barrier, inc=1, device_id={"cy": z + 1}, device_id_type=MESH)

    for p in range(NX):
        @pl.when((z > 0) & (z <= FAR))
        def _():
            pl.semaphore_signal(barrier, inc=1, device_id={"cy": I(0), "cx": mod(j + p)}, device_id_type=MESH)

        @pl.when(z == 0)
        def _():
            for zz in SHARE:
                pl.semaphore_signal(barrier, inc=1, device_id={"cy": I(zz), "cx": mod(j + p)}, device_id_type=MESH)

    def by_z(values):
        x = I(values[-1])
        for zz in range(NZ - 1):
            x = jnp.where(z == zz, I(values[zz]), x)
        return x

    lists = [[pack(u) for u in units(zz)] for zz in range(NZ)]
    count = by_z([len(x) for x in lists])
    codes = [by_z([x[min(i, len(x) - 1)] for x in lists]) for i in range(max(map(len, lists)))]

    def fields(u):
        x = codes[-1]
        for i, code in enumerate(codes[:-1]):
            x = jnp.where(u == i, code, x)
        return unpack(x)

    pl.semaphore_wait(barrier, NX - 1 + by_z([NX * FAR, NX + 1, NX + 2, 1]))

    def pair(g, kind, part, owner, dest):
        half = pl.ds(part * pc, pc)
        at = span(part, owner)
        if kind == 0:
            return k.at[SLOTS * dest + g, half, :], kb.at[g, chunk(part), at, :]
        if kind == 1:
            return v.at[SLOTS * dest + g, :, half], vb.at[g, chunk(part), :, at]
        return q.at[pl.ds(GQ * (SLOTS * dest + g), GQ), half, :], qb.at[2 * g + part, :, at, :]

    def xcopy(g, kind, part, p, owner, dest):
        src, dst = pair(g, kind, part, owner, dest)
        return pltpu.make_async_remote_copy(
            src_ref=src, dst_ref=dst, send_sem=xsend.at[g, kind, part, p - 1], recv_sem=xrecv.at[g, kind, part, p - 1],
            device_id={"cx": dest}, device_id_type=MESH)

    def xlocal(g, kind, part):
        src, dst = pair(g, kind, part, j, j)
        return pltpu.make_async_copy(src, dst, xloc.at[g, kind, part])

    for g in range(SLOTS):
        for kinds in ((0, 1), (2,)):
            for part in range(2):
                for p in range(1, NX):
                    for kind in kinds:
                        xcopy(g, kind, part, p, j, mod(j + p)).start()
                for kind in kinds:
                    xlocal(g, kind, part).start()

    def xwait(g, kinds, parts=(0, 1)):
        for part in parts:
            for kind in kinds:
                xlocal(g, kind, part).wait()
                for p in range(1, NX):
                    xcopy(g, kind, part, p, mod(j - p), j).wait_recv()

    def shift(zz):
        return pltpu.make_async_remote_copy(
            src_ref=qb.at[3, pl.ds(*SHARE[zz])], dst_ref=qb.at[SHIFT, pl.ds(0, SHARE[zz][1])], send_sem=qsend.at[zz - 1], recv_sem=qrecv.at[0],
            device_id={"cy": I(zz)}, device_id_type=MESH)

    def zcopies(g, ch, dz, send):
        return [
            pltpu.make_async_remote_copy(
                src_ref=buf.at[g, ch], dst_ref=buf.at[g, ch], send_sem=send.at[g, ch, i], recv_sem=zrecv.at[g, ch, i],
                device_id={"cy": z + dz}, device_id_type=MESH)
            for i, buf in enumerate((kb, vb))
        ]

    def goes_down(g):
        return z > jnp.where(g == 1, 1, 0)

    def down(g, ch):
        @pl.when(goes_down(g))
        def _():
            for d in zcopies(g, ch, -1, dsend):
                d.start()

    def up(g, ch):
        @pl.when(z < jnp.where(ch < NZ, NZ - 1, FAR))
        def _():
            for d in zcopies(g, ch, 1, usend):
                d.start()

    m[...] = jnp.full_like(m, -jnp.inf)
    l[...] = jnp.zeros_like(l)

    @pl.loop(0, 5)
    def _(i):
        a[i] = jnp.zeros(a.shape[1:], a.dtype)

    def begin(g):
        xwait(g, (0, 1))
        for ch in (z, TOP - z):
            down(I(g), ch)
        up(I(g), z)
        if g == 1:
            pl.when(z != 1)(lambda: up(I(g), TOP - z))

    def before(f):
        @pl.loop(0, 3)
        def _(i):
            act = jnp.where(i == 0, f[7], jnp.where(i == 1, f[8], f[9]))
            pl.when(act == KV1)(lambda: begin(1))
            pl.when(act == HIGH)(lambda: xwait(0, (2,), (1,)))

            @pl.when(act == QUERY)
            def _():
                xwait(1, (2,))

                @pl.when(z == 0)
                def _():
                    for zz in SHARE:
                        shift(zz).start()

            @pl.when(act == EXTRA)
            def _():
                for zz in SHARE:
                    pl.when(z == zz)(lambda: shift(zz).wait_recv())

            @pl.when((act >= LAND) & (act < HIGH))
            def _():
                g = lax.div(act - LAND, I(2 * NZ))
                ch = lax.rem(jnp.maximum(act - LAND, 0), I(2 * NZ))
                source = jnp.where(ch < NZ, ch, TOP - ch)

                @pl.when(source < z)
                def _():
                    for d in zcopies(g, ch, 1, usend):
                        d.wait_recv()
                    up(g, ch)
                    pl.when((z == 1) & (g == 1) & (ch == 0))(lambda: up(I(1), TOP - z))

                @pl.when(source > z)
                def _():
                    for d in zcopies(g, ch, -1, dsend):
                        d.wait_recv()
                    down(g, ch)

    def opiece(g, part, owner, dest, heads, hd, shifted):
        qs, to = (SHIFT, hd + 2 * (z - 1)) if shifted else (2 * g + part, hd)
        return dict(
            src_ref=ost.at[qs, pl.ds(hd, heads), span(part, dest), :],
            dst_ref=o.at[pl.ds(GQ * (SLOTS * owner + g) + to, heads), pl.ds(part * pc, pc), :])

    def oremote(g, part, p, owner, dest, heads=GQ, hd=0, shifted=False):
        return pltpu.make_async_remote_copy(
            **opiece(g, part, owner, dest, heads, hd, shifted),
            send_sem=osend.at[SHIFT if shifted else 2 * g + part, p], recv_sem=orecv.at[2 * g + part, p],
            device_id={"cy": I(0) if shifted else z, "cx": dest}, device_id_type=MESH)

    def olocal(g, part, heads=GQ, hd=0):
        r = opiece(g, part, j, j, heads, hd, False)
        return pltpu.make_async_copy(r["src_ref"], r["dst_ref"], osend.at[2 * g + part, 0])

    def finish(qs, n):
        y = a[qs, n] / jnp.sum(l[qs, n], axis=0, keepdims=True)
        at = pl.ds(pl.multiple_of(lax.rem(n, I(tiles)) * tq, tq), tq)
        ost[qs, lax.div(n, I(tiles)), at, :] = y.astype(ost.dtype).T

    def give_back(qs, n):
        hd = lax.div(n, I(tiles))
        for case in range(5):
            @pl.when(qs == case)
            def _():
                shifted = case == SHIFT
                g, part = (1, 1) if shifted else (case // 2, case % 2)
                for e in range(tq // pc):
                    at = lax.rem(n, I(tiles)) * (tq // pc) + e
                    dest = pos(part, at)
                    p = mod(dest - j)
                    if shifted:
                        oremote(g, part, p, j, dest, 1, hd, True).start()
                    else:
                        pl.when(p == 0)(lambda: olocal(g, part, 1, hd).start())
                        pl.when(p > 0)(lambda: oremote(g, part, p, j, dest, 1, hd).start())

    def after(f, h, w, hw):
        @pl.when(f[4] == 1)
        def _():
            for e in range(tiles):
                finish(f[0], tiles * h + e)

        @pl.when(w[4] == 1)
        def _():
            for e in range(tiles):
                give_back(w[0], tiles * hw + e)

    bufs = ((sa, xa), (sb, xb))

    def nxt(f, h, e, par, masked):
        rows = (e + 1) * tq if masked else kb.shape[2]
        sx, xx = bufs[par]
        return qb[f[0], h, pl.ds(e * tq, tq), :], kb.at[f[1], f[2]], sx.at[e], xx.at[e], e * tq if masked else None, rows

    def step(fn, hn, f, h, parity):
        qs = f[0]
        for par in range(2):
            for m_cur in (False, True):
                for m_nxt in (False, True):
                    @pl.when((parity == par) & (f[3] == int(m_cur)) & (fn[3] == int(m_nxt)))
                    def _():
                        for e in range(tiles):
                            n = tiles * h + e
                            sx, xx = bufs[par]
                            keys = (e + 1) * tq if m_cur else kb.shape[2]
                            stage(c, nxt(fn, hn, e, 1 - par, m_nxt),
                                  (sx.at[e], xx.at[e], vb.at[f[1], f[2]], m.at[qs, n], l.at[qs, n], a.at[qs, n], keys))

    first = fields(I(0))
    begin(0)
    xwait(0, (2,), (0,))
    before(first)
    for e in range(tiles):
        stage(c, nxt(first, I(0), e, 0, True), None)

    @pl.loop(0, count)
    def _(u):
        f = fields(u)
        fn = fields(jnp.minimum(u + 1, count - 1))
        w = fields(jnp.maximum(u - 1, 0))
        w[4] = jnp.where(u > 0, w[4], 0)

        @pl.loop(0, f[5])
        def _(h):
            wrap = h == f[5] - 1
            pl.when(wrap & (u + 1 < count))(lambda: before(fn))
            step([jnp.where(wrap, p, q) for p, q in zip(fn, f)], jnp.where(wrap, fn[10], f[10] + h + 1), f, f[10] + h,
                 lax.rem(f[6] + h, I(2)))
            after(f, f[10] + h, [jnp.where(h == 0, p, q) for p, q in zip(w, f)],
                  jnp.where(h == 0, w[10] + w[5] - 1, f[10] + h - 1))

    for g in range(SLOTS):
        for part in range(2):
            for p in range(1, NX):
                for kind in range(3):
                    xcopy(g, kind, part, p, j, mod(j + p)).wait_send()
    end = fields(count - 1)
    for e in range(tiles):
        give_back(end[0], tiles * (end[10] + end[5] - 1) + e)
    for g in range(SLOTS):
        for s in range(NZ):
            @pl.when(goes_down(g) & (s >= z))
            def _():
                for ch in (s, TOP - s):
                    for d in zcopies(g, ch, -1, dsend):
                        d.wait_send()

            @pl.when((z < NZ - 1) & (s <= z))
            def _():
                for d in zcopies(g, s, 1, usend):
                    d.wait_send()

            if g == 1:
                @pl.when((z < FAR) & (s <= z))
                def _():
                    for d in zcopies(g, TOP - s, 1, usend):
                        d.wait_send()
        for part in range(2):
            def keep():
                olocal(g, part).wait()
                for p in range(1, NX):
                    oremote(g, part, p, j, mod(j + p)).wait_send()
                    oremote(g, part, p, mod(j - p), j).wait_recv()

            def given():
                for p in range(NX):
                    oremote(g, part, p, mod(j - p), j).wait_recv()

            if g == 1 and part == 1:
                pl.when(z == 0)(given)
                pl.when(z > 0)(keep)
            else:
                keep()

    @pl.when(z == 0)
    def _():
        for zz in SHARE:
            shift(zz).wait_send()

    for zz in SHARE:
        @pl.when(z == zz)
        def _():
            for p in range(NX):
                oremote(1, 1, p, j, mod(j + p), SHARE[zz][1], shifted=True).wait_send()


def solution(mesh):
    assert mesh.shape["cx"] == NX and mesh.shape["cy"] == NZ
    spec = P(("batch", "cy", "cx"), None, None)

    def local(q, k, v):
        t, h, d = q.shape
        pc = t // 2
        rows = NX * pc
        c = d ** -0.5 * math.log2(math.e)
        tq = 2 * pc
        tiles = rows // tq
        f32, bf = jnp.float32, jnp.bfloat16
        dma = pltpu.SemaphoreType.DMA
        ot = pl.pallas_call(
            functools.partial(kernel, c),
            out_shape=jax.ShapeDtypeStruct((h, t, d), bf),
            in_specs=[pl.BlockSpec(memory_space=pl.ANY)] * 3,
            out_specs=pl.BlockSpec(memory_space=pl.ANY),
            scratch_shapes=[
                pltpu.VMEM((5, GQ, rows, d), bf),
                pltpu.VMEM((SLOTS, 2 * NZ, rows, d), bf),
                pltpu.VMEM((SLOTS, 2 * NZ, d, rows), bf),
                pltpu.VMEM((5, GQ * tiles, 1, tq), f32),
                pltpu.VMEM((5, GQ * tiles, 8, tq), f32),
                pltpu.VMEM((5, GQ * tiles, d, tq), f32),
                pltpu.VMEM((5, GQ, rows, d), bf),
                pltpu.VMEM((tiles, rows, tq), f32),
                pltpu.VMEM((tiles, rows, tq), f32),
                pltpu.VMEM((tiles, 8, tq), f32),
                pltpu.VMEM((tiles, 8, tq), f32),
                dma((SLOTS, 3, 2, NX - 1)),
                dma((SLOTS, 3, 2, NX - 1)),
                dma((SLOTS, 3, 2)),
                dma((NZ - 1,)),
                dma((1,)),
                dma((SLOTS, 2 * NZ, 2)),
                dma((SLOTS, 2 * NZ, 2)),
                dma((SLOTS, 2 * NZ, 2)),
                dma((5, NX)),
                dma((4, NX)),
            ],
            compiler_params=pltpu.CompilerParams(
                collective_id=0, has_side_effects=True, vmem_limit_bytes=38 * 2**20),
        )(jnp.transpose(q, (1, 0, 2)), jnp.transpose(k, (1, 0, 2)), jnp.transpose(v, (1, 2, 0)))
        return jnp.transpose(ot, (1, 0, 2))

    return jax.shard_map(local, mesh=mesh, in_specs=(spec, spec, spec), out_specs=spec, check_vma=False)
```

```python
import functools
import math

import jax
import jax.numpy as jnp
from jax import lax
from jax.experimental import pallas as pl
from jax.experimental.pallas import tpu as pltpu
from jax.sharding import PartitionSpec as P


NX = 4
NZ = 4
SLOTS = 2
GQ = 3
NB = 4
NT = (((1,), (1,)), ((), ()))
MESH = pl.DeviceIdType.MESH
I = jnp.int32


def stage(c, nxt, cur):
    qn, kn_ref, s_nxt, x_nxt, base, rows = nxt
    tq = qn.shape[0]
    bk = kn_ref.shape[0] // NB
    blocks = rows // bk
    if cur is not None:
        s_cur, x_cur, v_ref, m_ref, l_ref, a_ref, keys = cur
        blocks = max(blocks, keys // bk)
        m0 = m_ref[...]
        m1 = jnp.maximum(m0, jnp.max(x_cur[...], axis=0, keepdims=True))
        al = jnp.exp2((m0 - m1) * c)
        m_ref[...] = m1
        lsum = l_ref[...] * al
    xm = o = None
    for b in range(blocks):
        r = slice(b * bk, (b + 1) * bk)
        if b * bk < rows:
            s = lax.dot_general(kn_ref[r, :], qn, NT, preferred_element_type=jnp.float32)
            if base is not None and (b + 1) * bk > base:
                kk = lax.broadcasted_iota(I, s.shape, 0) + b * bk
                qq = lax.broadcasted_iota(I, s.shape, 1) + base
                s = jnp.where(kk <= qq, s, -jnp.inf)
            s_nxt[r, :] = s
            y = jnp.max(s.reshape(bk // 8, 8, tq), axis=0)
            xm = y if xm is None else jnp.maximum(xm, y)
        if cur is not None and b * bk < keys:
            p = jnp.exp2((s_cur[r, :] - m1) * c)
            lsum = lsum + jnp.sum(p.reshape(bk // 8, 8, tq), axis=0)
            d = jnp.dot(v_ref[:, r], p.astype(jnp.bfloat16), preferred_element_type=jnp.float32)
            o = d if o is None else o + d
    x_nxt[...] = xm
    if cur is not None:
        l_ref[...] = lsum
        a_ref[...] = a_ref[...] * al + o


SHIFT = 4
SHARE = {1: (0, 2), 2: (2, 1)}
FAR = max(SHARE)
TOP = 2 * NZ - 1
KV1, QUERY, EXTRA, LAND, HIGH = 1, 2, 3, 4, 20
RADIX = (5, 2, 8, 2, 2, 4, 2, 21, 21, 21, 3)

LOW_KV, HIGH_KV, LOW_Q, HIGH_Q, KV1_HERE, Q1_HERE = 9.5, 15, 24, 32, 43, 60
CHUNK, HOP, STEP = 11.25, 1.5, 1.28


def slot(qs):
    return 1 if qs == SHIFT else qs // 2


def diagonal(z, qs):
    return TOP if qs == SHIFT else z if qs % 2 == 0 else TOP - z


def plan():
    free, shifted, out, pend = {}, {}, [[] for _ in range(NZ)], [[] for _ in range(NZ)]
    landing = [{} for _ in range(NZ)]
    got = [set() for _ in range(NZ)]
    done = [set() for _ in range(NZ)]
    now = [LOW_Q] * NZ
    todo = []

    def wire(link, t, dur):
        free[link] = max(t, free.get(link, 0)) + dur
        return free[link] + HOP

    def travel(z, g, ch, t, dz):
        if dz < 0 and z > g or dz > 0 and z < (NZ - 1 if ch < NZ else FAR):
            landing[z + dz][g, ch] = wire((dz, z), t, CHUNK)

    def begin(z, g, low, high):
        for ch, t in ((z, low), (TOP - z, high)):
            got[z].add((g, ch))
            travel(z, g, ch, t, -1)
        travel(z, g, z, low, 1)
        if g == 1 and z != 1:
            travel(z, g, TOP - z, high, 1)

    def act(z, a, t):
        pend[z].append(a)
        done[z].add(a)
        if a == KV1:
            begin(z, 1, t, t)
        elif a == QUERY and z == 0:
            for zz, (_, heads) in SHARE.items():
                shifted[zz] = wire((1, 0), t, CHUNK * heads / 2) + 8 * (zz - 1)
        elif LAND <= a < HIGH:
            g, ch = (a - LAND) // (2 * NZ), (a - LAND) % (2 * NZ)
            got[z].add((g, ch))
            travel(z, g, ch, t, 1 if min(ch, TOP - ch) < z else -1)
            if z == 1 and (g, ch) == (1, 0):
                travel(z, 1, TOP - z, t, 1)

    def waiting(z):
        p = [(t, LAND + 2 * NZ * g + ch) for (g, ch), t in landing[z].items() if (g, ch) not in got[z]]
        p += [(t, a) for a, t in ((HIGH, HIGH_Q), (KV1, KV1_HERE)) if a not in done[z]]
        if KV1 in done[z] and QUERY not in done[z]:
            p.append((Q1_HERE, QUERY))
        if z in shifted and EXTRA not in done[z]:
            p.append((shifted[z], EXTRA))
        return sorted(p)

    def ready(z, qs, ch):
        need = {1: HIGH, 2: QUERY, 3: QUERY, SHIFT: EXTRA}.get(qs)
        return (need is None or need in done[z]) and (slot(qs), ch) in got[z]

    for z in range(NZ):
        sets = [0, 1, 2] + [3] * (z > 0) + [SHIFT] * (z in SHARE)
        todo.append([(qs, ch) for qs in sets for ch in range(diagonal(z, qs) + 1)])
        begin(z, 0, LOW_KV, HIGH_KV)
    while any(todo):
        z = min((z for z in range(NZ) if todo[z]), key=lambda z: now[z])
        for t, a in waiting(z):
            if t <= now[z] and len(pend[z]) < 3:
                act(z, a, now[z])
        can = [u for u in todo[z] if ready(z, *u)]
        if can:
            rank = (0, 2, 1, 4, 3) if z == 0 else (0, 1, 3, 4, 2)
            qs, ch = min(can, key=lambda u: (rank[u[0]], u[1] != diagonal(z, u[0]), u[1] if u[1] < diagonal(z, u[0]) else -u[1]))
            todo[z].remove((qs, ch))
            out[z].append((qs, ch, *pend[z]))
            pend[z] = []
            now[z] += STEP * (SHARE[z][1] if qs == SHIFT else GQ)
        else:
            coming = waiting(z)
            if coming and len(pend[z]) < 3:
                now[z] = max(now[z], coming[0][0])
                act(z, coming[0][1], now[z])
            else:
                now[z] += 0.5
    assert not any(pend)
    return out, now


def units(z):
    work = plan()[0][z]
    if z > 0:
        k = len(work)
        while work[k - 1][0] == 3 and len(work[k - 1]) == 2 and len(work) - k < 3:
            k -= 1
        work = [(w, 0, SHARE[z][1] if w[0] == SHIFT else GQ) for w in work[:k]] + [
            (w, h, 1) for h in range(GQ) for w in work[k:]]
    else:
        work = [(w, 0, GQ) for w in work]
    last = {(w[0], h): i for i, (w, h0, n) in enumerate(work) for h in range(h0, h0 + n)}
    out = []
    steps = 0
    for i, ((qs, ch, *acts), h0, heads) in enumerate(work):
        ends = [last[qs, h] == i for h in range(h0, h0 + heads)]
        assert all(ends) or not any(ends)
        out.append((qs, slot(qs), ch, int(ch == diagonal(z, qs)), int(ends[0]), heads, steps % 2,
                    *acts, *[0] * (3 - len(acts)), h0))
        steps += heads
    return out


def pack(u):
    x = 0
    for r, f in zip(RADIX, u):
        x = x * r + f
    return x


def unpack(x):
    out = []
    for r in RADIX[::-1]:
        out.append(lax.rem(x, I(r)))
        x = lax.div(x, I(r))
    return out[::-1]


def kernel(c, q, k, v, o, qb, kb, vb, m, l, a, ost, sa, sb, xa, xb,
           xsend, xrecv, xloc, qsend, qrecv, zrecv, dsend, usend, osend, orecv):
    z = lax.axis_index("cy")
    j = lax.axis_index("cx")
    pc = k.shape[1] // 2
    tq = sa.shape[2]
    tiles = qb.shape[2] // tq

    def mod(x):
        return lax.rem(x + 2 * NX, I(NX))

    def chunk(part):
        return z if part == 0 else TOP - z

    def pos(part, jj):
        return jj if part == 0 else NX - 1 - jj

    def span(part, jj):
        return pl.ds(pl.multiple_of(pos(part, jj) * pc, pc), pc)

    barrier = pltpu.get_barrier_semaphore()
    for p in range(1, NX):
        pl.semaphore_signal(barrier, inc=1, device_id={"cx": mod(j + p)}, device_id_type=MESH)

    @pl.when(z > 1)
    def _():
        pl.semaphore_signal(barrier, inc=1, device_id={"cy": z - 1}, device_id_type=MESH)

    @pl.when((z > 0) & (z < NZ - 1))
    def _():
        pl.semaphore_signal(barrier, inc=1, device_id={"cy": z + 1}, device_id_type=MESH)

    for p in range(NX):
        @pl.when((z > 0) & (z <= FAR))
        def _():
            pl.semaphore_signal(barrier, inc=1, device_id={"cy": I(0), "cx": mod(j + p)}, device_id_type=MESH)

        @pl.when(z == 0)
        def _():
            for zz in SHARE:
                pl.semaphore_signal(barrier, inc=1, device_id={"cy": I(zz), "cx": mod(j + p)}, device_id_type=MESH)

    def by_z(values):
        x = I(values[-1])
        for zz in range(NZ - 1):
            x = jnp.where(z == zz, I(values[zz]), x)
        return x

    lists = [[pack(u) for u in units(zz)] for zz in range(NZ)]
    count = by_z([len(x) for x in lists])
    codes = [by_z([x[min(i, len(x) - 1)] for x in lists]) for i in range(max(map(len, lists)))]

    def fields(u):
        x = codes[-1]
        for i, code in enumerate(codes[:-1]):
            x = jnp.where(u == i, code, x)
        return unpack(x)

    pl.semaphore_wait(barrier, NX - 1 + by_z([NX * FAR, NX + 1, NX + 2, 1]))

    def pair(g, kind, part, owner, dest):
        half = pl.ds(part * pc, pc)
        at = span(part, owner)
        if kind == 0:
            return k.at[SLOTS * dest + g, half, :], kb.at[g, chunk(part), at, :]
        if kind == 1:
            return v.at[SLOTS * dest + g, :, half], vb.at[g, chunk(part), :, at]
        return q.at[pl.ds(GQ * (SLOTS * dest + g), GQ), half, :], qb.at[2 * g + part, :, at, :]

    def xcopy(g, kind, part, p, owner, dest):
        src, dst = pair(g, kind, part, owner, dest)
        return pltpu.make_async_remote_copy(
            src_ref=src, dst_ref=dst, send_sem=xsend.at[g, kind, part, p - 1], recv_sem=xrecv.at[g, kind, part, p - 1],
            device_id={"cx": dest}, device_id_type=MESH)

    def xlocal(g, kind, part):
        src, dst = pair(g, kind, part, j, j)
        return pltpu.make_async_copy(src, dst, xloc.at[g, kind, part])

    for g in range(SLOTS):
        for kinds in ((0, 1), (2,)):
            for part in range(2):
                for p in range(1, NX):
                    for kind in kinds:
                        xcopy(g, kind, part, p, j, mod(j + p)).start()
                for kind in kinds:
                    xlocal(g, kind, part).start()

    def xwait(g, kinds, parts=(0, 1)):
        for part in parts:
            for kind in kinds:
                xlocal(g, kind, part).wait()
                for p in range(1, NX):
                    xcopy(g, kind, part, p, mod(j - p), j).wait_recv()

    def shift(zz):
        return pltpu.make_async_remote_copy(
            src_ref=qb.at[3, pl.ds(*SHARE[zz])], dst_ref=qb.at[SHIFT, pl.ds(0, SHARE[zz][1])], send_sem=qsend.at[zz - 1], recv_sem=qrecv.at[0],
            device_id={"cy": I(zz)}, device_id_type=MESH)

    def zcopies(g, ch, dz, send):
        return [
            pltpu.make_async_remote_copy(
                src_ref=buf.at[g, ch], dst_ref=buf.at[g, ch], send_sem=send.at[g, ch, i], recv_sem=zrecv.at[g, ch, i],
                device_id={"cy": z + dz}, device_id_type=MESH)
            for i, buf in enumerate((kb, vb))
        ]

    def goes_down(g):
        return z > jnp.where(g == 1, 1, 0)

    def down(g, ch):
        @pl.when(goes_down(g))
        def _():
            for d in zcopies(g, ch, -1, dsend):
                d.start()

    def up(g, ch):
        @pl.when(z < jnp.where(ch < NZ, NZ - 1, FAR))
        def _():
            for d in zcopies(g, ch, 1, usend):
                d.start()

    m[...] = jnp.full_like(m, -jnp.inf)
    l[...] = jnp.zeros_like(l)

    @pl.loop(0, 5)
    def _(i):
        a[i] = jnp.zeros(a.shape[1:], a.dtype)

    def begin(g):
        xwait(g, (0, 1), (0,))
        down(I(g), z)
        up(I(g), z)
        xwait(g, (0, 1), (1,))
        down(I(g), TOP - z)
        if g == 1:
            pl.when(z != 1)(lambda: up(I(g), TOP - z))

    def before(f):
        @pl.loop(0, 3)
        def _(i):
            act = jnp.where(i == 0, f[7], jnp.where(i == 1, f[8], f[9]))
            pl.when(act == KV1)(lambda: begin(1))
            pl.when(act == HIGH)(lambda: xwait(0, (2,), (1,)))

            @pl.when(act == QUERY)
            def _():
                xwait(1, (2,))

                @pl.when(z == 0)
                def _():
                    for zz in SHARE:
                        shift(zz).start()

            @pl.when(act == EXTRA)
            def _():
                for zz in SHARE:
                    pl.when(z == zz)(lambda: shift(zz).wait_recv())

            @pl.when((act >= LAND) & (act < HIGH))
            def _():
                g = lax.div(act - LAND, I(2 * NZ))
                ch = lax.rem(jnp.maximum(act - LAND, 0), I(2 * NZ))
                source = jnp.where(ch < NZ, ch, TOP - ch)

                @pl.when(source < z)
                def _():
                    for d in zcopies(g, ch, 1, usend):
                        d.wait_recv()
                    up(g, ch)
                    pl.when((z == 1) & (g == 1) & (ch == 0))(lambda: up(I(1), TOP - z))

                @pl.when(source > z)
                def _():
                    for d in zcopies(g, ch, -1, dsend):
                        d.wait_recv()
                    down(g, ch)

    def opiece(g, part, owner, dest, heads, hd, shifted):
        qs, to = (SHIFT, hd + 2 * (z - 1)) if shifted else (2 * g + part, hd)
        return dict(
            src_ref=ost.at[qs, pl.ds(hd, heads), span(part, dest), :],
            dst_ref=o.at[pl.ds(GQ * (SLOTS * owner + g) + to, heads), pl.ds(part * pc, pc), :])

    def oremote(g, part, p, owner, dest, heads=GQ, hd=0, shifted=False):
        return pltpu.make_async_remote_copy(
            **opiece(g, part, owner, dest, heads, hd, shifted),
            send_sem=osend.at[SHIFT if shifted else 2 * g + part, p], recv_sem=orecv.at[2 * g + part, p],
            device_id={"cy": I(0) if shifted else z, "cx": dest}, device_id_type=MESH)

    def olocal(g, part, heads=GQ, hd=0):
        r = opiece(g, part, j, j, heads, hd, False)
        return pltpu.make_async_copy(r["src_ref"], r["dst_ref"], osend.at[2 * g + part, 0])

    def finish(qs, n):
        y = a[qs, n] / jnp.sum(l[qs, n], axis=0, keepdims=True)
        at = pl.ds(pl.multiple_of(lax.rem(n, I(tiles)) * tq, tq), tq)
        ost[qs, lax.div(n, I(tiles)), at, :] = y.astype(ost.dtype).T

    def give_back(qs, n):
        hd = lax.div(n, I(tiles))
        for case in range(5):
            @pl.when(qs == case)
            def _():
                shifted = case == SHIFT
                g, part = (1, 1) if shifted else (case // 2, case % 2)
                for e in range(tq // pc):
                    at = lax.rem(n, I(tiles)) * (tq // pc) + e
                    dest = pos(part, at)
                    p = mod(dest - j)
                    if shifted:
                        oremote(g, part, p, j, dest, 1, hd, True).start()
                    else:
                        pl.when(p == 0)(lambda: olocal(g, part, 1, hd).start())
                        pl.when(p > 0)(lambda: oremote(g, part, p, j, dest, 1, hd).start())

    def after(f, h, w, hw):
        @pl.when(f[4] == 1)
        def _():
            for e in range(tiles):
                finish(f[0], tiles * h + e)

        @pl.when(w[4] == 1)
        def _():
            for e in range(tiles):
                give_back(w[0], tiles * hw + e)

    bufs = ((sa, xa), (sb, xb))

    def nxt(f, h, e, par, masked):
        rows = (e + 1) * tq if masked else kb.shape[2]
        sx, xx = bufs[par]
        return qb[f[0], h, pl.ds(e * tq, tq), :], kb.at[f[1], f[2]], sx.at[e], xx.at[e], e * tq if masked else None, rows

    def step(fn, hn, f, h, parity):
        qs = f[0]
        for par in range(2):
            for m_cur in (False, True):
                for m_nxt in (False, True):
                    @pl.when((parity == par) & (f[3] == int(m_cur)) & (fn[3] == int(m_nxt)))
                    def _():
                        for e in range(tiles):
                            n = tiles * h + e
                            sx, xx = bufs[par]
                            keys = (e + 1) * tq if m_cur else kb.shape[2]
                            stage(c, nxt(fn, hn, e, 1 - par, m_nxt),
                                  (sx.at[e], xx.at[e], vb.at[f[1], f[2]], m.at[qs, n], l.at[qs, n], a.at[qs, n], keys))

    first = fields(I(0))
    begin(0)
    xwait(0, (2,), (0,))
    before(first)
    for e in range(tiles):
        stage(c, nxt(first, I(0), e, 0, True), None)

    @pl.loop(0, count)
    def _(u):
        f = fields(u)
        fn = fields(jnp.minimum(u + 1, count - 1))
        w = fields(jnp.maximum(u - 1, 0))
        w[4] = jnp.where(u > 0, w[4], 0)

        @pl.loop(0, f[5])
        def _(h):
            wrap = h == f[5] - 1
            pl.when(wrap & (u + 1 < count))(lambda: before(fn))
            step([jnp.where(wrap, p, q) for p, q in zip(fn, f)], jnp.where(wrap, fn[10], f[10] + h + 1), f, f[10] + h,
                 lax.rem(f[6] + h, I(2)))
            after(f, f[10] + h, [jnp.where(h == 0, p, q) for p, q in zip(w, f)],
                  jnp.where(h == 0, w[10] + w[5] - 1, f[10] + h - 1))

    for g in range(SLOTS):
        for part in range(2):
            for p in range(1, NX):
                for kind in range(3):
                    xcopy(g, kind, part, p, j, mod(j + p)).wait_send()
    end = fields(count - 1)
    for e in range(tiles):
        give_back(end[0], tiles * (end[10] + end[5] - 1) + e)
    for g in range(SLOTS):
        for s in range(NZ):
            @pl.when(goes_down(g) & (s >= z))
            def _():
                for ch in (s, TOP - s):
                    for d in zcopies(g, ch, -1, dsend):
                        d.wait_send()

            @pl.when((z < NZ - 1) & (s <= z))
            def _():
                for d in zcopies(g, s, 1, usend):
                    d.wait_send()

            if g == 1:
                @pl.when((z < FAR) & (s <= z))
                def _():
                    for d in zcopies(g, TOP - s, 1, usend):
                        d.wait_send()
        for part in range(2):
            def keep():
                olocal(g, part).wait()
                for p in range(1, NX):
                    oremote(g, part, p, j, mod(j + p)).wait_send()
                    oremote(g, part, p, mod(j - p), j).wait_recv()

            def given():
                for p in range(NX):
                    oremote(g, part, p, mod(j - p), j).wait_recv()

            if g == 1 and part == 1:
                pl.when(z == 0)(given)
                pl.when(z > 0)(keep)
            else:
                keep()

    @pl.when(z == 0)
    def _():
        for zz in SHARE:
            shift(zz).wait_send()

    for zz in SHARE:
        @pl.when(z == zz)
        def _():
            for p in range(NX):
                oremote(1, 1, p, j, mod(j + p), SHARE[zz][1], shifted=True).wait_send()


def solution(mesh):
    assert mesh.shape["cx"] == NX and mesh.shape["cy"] == NZ
    spec = P(("batch", "cy", "cx"), None, None)

    def local(q, k, v):
        t, h, d = q.shape
        pc = t // 2
        rows = NX * pc
        c = d ** -0.5 * math.log2(math.e)
        tq = 2 * pc
        tiles = rows // tq
        f32, bf = jnp.float32, jnp.bfloat16
        dma = pltpu.SemaphoreType.DMA
        ot = pl.pallas_call(
            functools.partial(kernel, c),
            out_shape=jax.ShapeDtypeStruct((h, t, d), bf),
            in_specs=[pl.BlockSpec(memory_space=pl.ANY)] * 3,
            out_specs=pl.BlockSpec(memory_space=pl.ANY),
            scratch_shapes=[
                pltpu.VMEM((5, GQ, rows, d), bf),
                pltpu.VMEM((SLOTS, 2 * NZ, rows, d), bf),
                pltpu.VMEM((SLOTS, 2 * NZ, d, rows), bf),
                pltpu.VMEM((5, GQ * tiles, 1, tq), f32),
                pltpu.VMEM((5, GQ * tiles, 8, tq), f32),
                pltpu.VMEM((5, GQ * tiles, d, tq), f32),
                pltpu.VMEM((5, GQ, rows, d), bf),
                pltpu.VMEM((tiles, rows, tq), f32),
                pltpu.VMEM((tiles, rows, tq), f32),
                pltpu.VMEM((tiles, 8, tq), f32),
                pltpu.VMEM((tiles, 8, tq), f32),
                dma((SLOTS, 3, 2, NX - 1)),
                dma((SLOTS, 3, 2, NX - 1)),
                dma((SLOTS, 3, 2)),
                dma((NZ - 1,)),
                dma((1,)),
                dma((SLOTS, 2 * NZ, 2)),
                dma((SLOTS, 2 * NZ, 2)),
                dma((SLOTS, 2 * NZ, 2)),
                dma((5, NX)),
                dma((4, NX)),
            ],
            compiler_params=pltpu.CompilerParams(
                collective_id=0, has_side_effects=True, vmem_limit_bytes=38 * 2**20),
        )(jnp.transpose(q, (1, 0, 2)), jnp.transpose(k, (1, 0, 2)), jnp.transpose(v, (1, 2, 0)))
        return jnp.transpose(ot, (1, 0, 2))

    return jax.shard_map(local, mesh=mesh, in_specs=(spec, spec, spec), out_specs=spec, check_vma=False)
```

```python
import functools
import math

import jax
import jax.numpy as jnp
from jax import lax
from jax.experimental import pallas as pl
from jax.experimental.pallas import tpu as pltpu
from jax.sharding import PartitionSpec as P


NX = 4
NZ = 4
SLOTS = 2
GQ = 3
NB = 4
NT = (((1,), (1,)), ((), ()))
MESH = pl.DeviceIdType.MESH
I = jnp.int32


def stage(c, nxt, cur):
    qn, kn_ref, s_nxt, x_nxt, base, rows = nxt
    tq = qn.shape[0]
    bk = kn_ref.shape[0] // NB
    blocks = rows // bk
    if cur is not None:
        s_cur, x_cur, v_ref, m_ref, l_ref, a_ref, keys = cur
        blocks = max(blocks, keys // bk)
        m0 = m_ref[...]
        m1 = jnp.maximum(m0, jnp.max(x_cur[...], axis=0, keepdims=True))
        al = jnp.exp2((m0 - m1) * c)
        m_ref[...] = m1
        lsum = l_ref[...] * al
    xm = o = None
    for b in range(blocks):
        r = slice(b * bk, (b + 1) * bk)
        if b * bk < rows:
            s = lax.dot_general(kn_ref[r, :], qn, NT, preferred_element_type=jnp.float32)
            if base is not None and (b + 1) * bk > base:
                kk = lax.broadcasted_iota(I, s.shape, 0) + b * bk
                qq = lax.broadcasted_iota(I, s.shape, 1) + base
                s = jnp.where(kk <= qq, s, -jnp.inf)
            s_nxt[r, :] = s
            y = jnp.max(s.reshape(bk // 8, 8, tq), axis=0)
            xm = y if xm is None else jnp.maximum(xm, y)
        if cur is not None and b * bk < keys:
            p = jnp.exp2((s_cur[r, :] - m1) * c)
            lsum = lsum + jnp.sum(p.reshape(bk // 8, 8, tq), axis=0)
            d = jnp.dot(v_ref[:, r], p.astype(jnp.bfloat16), preferred_element_type=jnp.float32)
            o = d if o is None else o + d
    x_nxt[...] = xm
    if cur is not None:
        l_ref[...] = lsum
        a_ref[...] = a_ref[...] * al + o


SHIFT = 4
SHARE = {1: (0, 2), 2: (2, 1)}
FAR = max(SHARE)
TOP = 2 * NZ - 1
KV1, QUERY, EXTRA, LAND, HIGH = 1, 2, 3, 4, 20
RADIX = (5, 2, 8, 2, 2, 4, 2, 21, 21, 21, 3)

LOW_KV, HIGH_KV, LOW_Q, HIGH_Q, KV1_HERE, Q1_HERE = 11, 17, 27, 36, 48, 66
CHUNK, HOP, STEP = 12, 3, 1.4


def slot(qs):
    return 1 if qs == SHIFT else qs // 2


def diagonal(z, qs):
    return TOP if qs == SHIFT else z if qs % 2 == 0 else TOP - z


def plan():
    free, shifted, out, pend = {}, {}, [[] for _ in range(NZ)], [[] for _ in range(NZ)]
    landing = [{} for _ in range(NZ)]
    got = [set() for _ in range(NZ)]
    done = [set() for _ in range(NZ)]
    now = [LOW_Q] * NZ
    todo = []

    def wire(link, t, dur):
        free[link] = max(t, free.get(link, 0)) + dur
        return free[link] + HOP

    def travel(z, g, ch, t, dz):
        if dz < 0 and z > g or dz > 0 and z < (NZ - 1 if ch < NZ else FAR):
            landing[z + dz][g, ch] = wire((dz, z), t, CHUNK)

    def begin(z, g, low, high):
        for ch, t in ((z, low), (TOP - z, high)):
            got[z].add((g, ch))
            travel(z, g, ch, t, -1)
        travel(z, g, z, low, 1)
        if g == 1 and z != 1:
            travel(z, g, TOP - z, high, 1)

    def act(z, a, t):
        pend[z].append(a)
        done[z].add(a)
        if a == KV1:
            begin(z, 1, t, t)
        elif a == QUERY and z == 0:
            for zz, (_, heads) in SHARE.items():
                shifted[zz] = wire((1, 0), t, CHUNK * heads / 2) + 8 * (zz - 1)
        elif LAND <= a < HIGH:
            g, ch = (a - LAND) // (2 * NZ), (a - LAND) % (2 * NZ)
            got[z].add((g, ch))
            travel(z, g, ch, t, 1 if min(ch, TOP - ch) < z else -1)
            if z == 1 and (g, ch) == (1, 0):
                travel(z, 1, TOP - z, t, 1)

    def waiting(z):
        p = [(t, LAND + 2 * NZ * g + ch) for (g, ch), t in landing[z].items() if (g, ch) not in got[z]]
        p += [(t, a) for a, t in ((HIGH, HIGH_Q), (KV1, KV1_HERE)) if a not in done[z]]
        if KV1 in done[z] and QUERY not in done[z]:
            p.append((Q1_HERE, QUERY))
        if z in shifted and EXTRA not in done[z]:
            p.append((shifted[z], EXTRA))
        return sorted(p)

    def ready(z, qs, ch):
        need = {1: HIGH, 2: QUERY, 3: QUERY, SHIFT: EXTRA}.get(qs)
        return (need is None or need in done[z]) and (slot(qs), ch) in got[z]

    for z in range(NZ):
        sets = [0, 1, 2] + [3] * (z > 0) + [SHIFT] * (z in SHARE)
        todo.append([(qs, ch) for qs in sets for ch in range(diagonal(z, qs) + 1)])
        begin(z, 0, LOW_KV, HIGH_KV)
    while any(todo):
        z = min((z for z in range(NZ) if todo[z]), key=lambda z: now[z])
        for t, a in waiting(z):
            if t <= now[z] and len(pend[z]) < 3:
                act(z, a, now[z])
        can = [u for u in todo[z] if ready(z, *u)]
        if can:
            rank = (0, 2, 1, 4, 3) if z == 0 else (0, 1, 3, 4, 2)
            qs, ch = min(can, key=lambda u: (rank[u[0]], u[1] != diagonal(z, u[0]), u[1] if u[1] < diagonal(z, u[0]) else -u[1]))
            todo[z].remove((qs, ch))
            out[z].append((qs, ch, *pend[z]))
            pend[z] = []
            now[z] += STEP * (SHARE[z][1] if qs == SHIFT else GQ)
        else:
            coming = waiting(z)
            if coming and len(pend[z]) < 3:
                now[z] = max(now[z], coming[0][0])
                act(z, coming[0][1], now[z])
            else:
                now[z] += 0.5
    assert not any(pend)
    return out, now


def units(z):
    work = plan()[0][z]
    if z > 0:
        k = len(work)
        while work[k - 1][0] == 3 and len(work[k - 1]) == 2 and len(work) - k < 3:
            k -= 1
        work = [(w, 0, SHARE[z][1] if w[0] == SHIFT else GQ) for w in work[:k]] + [
            (w, h, 1) for h in range(GQ) for w in work[k:]]
    else:
        work = [(w, 0, GQ) for w in work]
    last = {(w[0], h): i for i, (w, h0, n) in enumerate(work) for h in range(h0, h0 + n)}
    out = []
    steps = 0
    for i, ((qs, ch, *acts), h0, heads) in enumerate(work):
        ends = [last[qs, h] == i for h in range(h0, h0 + heads)]
        assert all(ends) or not any(ends)
        out.append((qs, slot(qs), ch, int(ch == diagonal(z, qs)), int(ends[0]), heads, steps % 2,
                    *acts, *[0] * (3 - len(acts)), h0))
        steps += heads
    return out


def pack(u):
    x = 0
    for r, f in zip(RADIX, u):
        x = x * r + f
    return x


def unpack(x):
    out = []
    for r in RADIX[::-1]:
        out.append(lax.rem(x, I(r)))
        x = lax.div(x, I(r))
    return out[::-1]


def kernel(c, q, k, v, o, qb, kb, vb, m, l, a, ost, sa, sb, xa, xb,
           xsend, xrecv, xloc, qsend, qrecv, zrecv, dsend, usend, osend, orecv):
    z = lax.axis_index("cy")
    j = lax.axis_index("cx")
    pc = k.shape[1] // 2
    tq = sa.shape[2]
    tiles = qb.shape[2] // tq

    def mod(x):
        return lax.rem(x + 2 * NX, I(NX))

    def chunk(part):
        return z if part == 0 else TOP - z

    def pos(part, jj):
        return jj if part == 0 else NX - 1 - jj

    def span(part, jj):
        return pl.ds(pl.multiple_of(pos(part, jj) * pc, pc), pc)

    barrier = pltpu.get_barrier_semaphore()
    for p in range(1, NX):
        pl.semaphore_signal(barrier, inc=1, device_id={"cx": mod(j + p)}, device_id_type=MESH)

    @pl.when(z > 1)
    def _():
        pl.semaphore_signal(barrier, inc=1, device_id={"cy": z - 1}, device_id_type=MESH)

    @pl.when((z > 0) & (z < NZ - 1))
    def _():
        pl.semaphore_signal(barrier, inc=1, device_id={"cy": z + 1}, device_id_type=MESH)

    for p in range(NX):
        @pl.when((z > 0) & (z <= FAR))
        def _():
            pl.semaphore_signal(barrier, inc=1, device_id={"cy": I(0), "cx": mod(j + p)}, device_id_type=MESH)

        @pl.when(z == 0)
        def _():
            for zz in SHARE:
                pl.semaphore_signal(barrier, inc=1, device_id={"cy": I(zz), "cx": mod(j + p)}, device_id_type=MESH)

    def by_z(values):
        x = I(values[-1])
        for zz in range(NZ - 1):
            x = jnp.where(z == zz, I(values[zz]), x)
        return x

    lists = [[pack(u) for u in units(zz)] for zz in range(NZ)]
    count = by_z([len(x) for x in lists])
    codes = [by_z([x[min(i, len(x) - 1)] for x in lists]) for i in range(max(map(len, lists)))]

    def fields(u):
        x = codes[-1]
        for i, code in enumerate(codes[:-1]):
            x = jnp.where(u == i, code, x)
        return unpack(x)

    pl.semaphore_wait(barrier, NX - 1 + by_z([NX * FAR, NX + 1, NX + 2, 1]))

    def pair(g, kind, part, owner, dest):
        half = pl.ds(part * pc, pc)
        at = span(part, owner)
        if kind == 0:
            return k.at[SLOTS * dest + g, half, :], kb.at[g, chunk(part), at, :]
        if kind == 1:
            return v.at[SLOTS * dest + g, :, half], vb.at[g, chunk(part), :, at]
        return q.at[pl.ds(GQ * (SLOTS * dest + g), GQ), half, :], qb.at[2 * g + part, :, at, :]

    def xcopy(g, kind, part, p, owner, dest):
        src, dst = pair(g, kind, part, owner, dest)
        return pltpu.make_async_remote_copy(
            src_ref=src, dst_ref=dst, send_sem=xsend.at[g, kind, part, p - 1], recv_sem=xrecv.at[g, kind, part, p - 1],
            device_id={"cx": dest}, device_id_type=MESH)

    def xlocal(g, kind, part):
        src, dst = pair(g, kind, part, j, j)
        return pltpu.make_async_copy(src, dst, xloc.at[g, kind, part])

    for g in range(SLOTS):
        for kinds in ((0, 1), (2,)):
            for part in range(2):
                for p in range(1, NX):
                    for kind in kinds:
                        xcopy(g, kind, part, p, j, mod(j + p)).start()
                for kind in kinds:
                    xlocal(g, kind, part).start()

    def xwait(g, kinds, parts=(0, 1)):
        for part in parts:
            for kind in kinds:
                xlocal(g, kind, part).wait()
                for p in range(1, NX):
                    xcopy(g, kind, part, p, mod(j - p), j).wait_recv()

    def shift(zz):
        return pltpu.make_async_remote_copy(
            src_ref=qb.at[3, pl.ds(*SHARE[zz])], dst_ref=qb.at[SHIFT, pl.ds(0, SHARE[zz][1])], send_sem=qsend.at[zz - 1], recv_sem=qrecv.at[0],
            device_id={"cy": I(zz)}, device_id_type=MESH)

    def zcopies(g, ch, dz, send):
        return [
            pltpu.make_async_remote_copy(
                src_ref=buf.at[g, ch], dst_ref=buf.at[g, ch], send_sem=send.at[g, ch, i], recv_sem=zrecv.at[g, ch, i],
                device_id={"cy": z + dz}, device_id_type=MESH)
            for i, buf in enumerate((kb, vb))
        ]

    def goes_down(g):
        return z > jnp.where(g == 1, 1, 0)

    def down(g, ch):
        @pl.when(goes_down(g))
        def _():
            for d in zcopies(g, ch, -1, dsend):
                d.start()

    def up(g, ch):
        @pl.when(z < jnp.where(ch < NZ, NZ - 1, FAR))
        def _():
            for d in zcopies(g, ch, 1, usend):
                d.start()

    m[...] = jnp.full_like(m, -jnp.inf)
    l[...] = jnp.zeros_like(l)

    @pl.loop(0, 5)
    def _(i):
        a[i] = jnp.zeros(a.shape[1:], a.dtype)

    def begin(g):
        xwait(g, (0, 1), (0,))
        down(I(g), z)
        up(I(g), z)
        xwait(g, (0, 1), (1,))
        down(I(g), TOP - z)
        if g == 1:
            pl.when(z != 1)(lambda: up(I(g), TOP - z))

    def before(f):
        @pl.loop(0, 3)
        def _(i):
            act = jnp.where(i == 0, f[7], jnp.where(i == 1, f[8], f[9]))
            pl.when(act == KV1)(lambda: begin(1))
            pl.when(act == HIGH)(lambda: xwait(0, (2,), (1,)))

            @pl.when(act == QUERY)
            def _():
                xwait(1, (2,))

                @pl.when(z == 0)
                def _():
                    for zz in SHARE:
                        shift(zz).start()

            @pl.when(act == EXTRA)
            def _():
                for zz in SHARE:
                    pl.when(z == zz)(lambda: shift(zz).wait_recv())

            @pl.when((act >= LAND) & (act < HIGH))
            def _():
                g = lax.div(act - LAND, I(2 * NZ))
                ch = lax.rem(jnp.maximum(act - LAND, 0), I(2 * NZ))
                source = jnp.where(ch < NZ, ch, TOP - ch)

                @pl.when(source < z)
                def _():
                    for d in zcopies(g, ch, 1, usend):
                        d.wait_recv()
                    up(g, ch)
                    pl.when((z == 1) & (g == 1) & (ch == 0))(lambda: up(I(1), TOP - z))

                @pl.when(source > z)
                def _():
                    for d in zcopies(g, ch, -1, dsend):
                        d.wait_recv()
                    down(g, ch)

    def opiece(g, part, owner, dest, heads, hd, shifted):
        qs, to = (SHIFT, hd + 2 * (z - 1)) if shifted else (2 * g + part, hd)
        return dict(
            src_ref=ost.at[qs, pl.ds(hd, heads), span(part, dest), :],
            dst_ref=o.at[pl.ds(GQ * (SLOTS * owner + g) + to, heads), pl.ds(part * pc, pc), :])

    def oremote(g, part, p, owner, dest, heads=GQ, hd=0, shifted=False):
        return pltpu.make_async_remote_copy(
            **opiece(g, part, owner, dest, heads, hd, shifted),
            send_sem=osend.at[SHIFT if shifted else 2 * g + part, p], recv_sem=orecv.at[2 * g + part, p],
            device_id={"cy": I(0) if shifted else z, "cx": dest}, device_id_type=MESH)

    def olocal(g, part, heads=GQ, hd=0):
        r = opiece(g, part, j, j, heads, hd, False)
        return pltpu.make_async_copy(r["src_ref"], r["dst_ref"], osend.at[2 * g + part, 0])

    def finish(qs, n):
        y = a[qs, n] / jnp.sum(l[qs, n], axis=0, keepdims=True)
        at = pl.ds(pl.multiple_of(lax.rem(n, I(tiles)) * tq, tq), tq)
        ost[qs, lax.div(n, I(tiles)), at, :] = y.astype(ost.dtype).T

    def give_back(qs, n):
        hd = lax.div(n, I(tiles))
        for case in range(5):
            @pl.when(qs == case)
            def _():
                shifted = case == SHIFT
                g, part = (1, 1) if shifted else (case // 2, case % 2)
                for e in range(tq // pc):
                    at = lax.rem(n, I(tiles)) * (tq // pc) + e
                    dest = pos(part, at)
                    p = mod(dest - j)
                    if shifted:
                        oremote(g, part, p, j, dest, 1, hd, True).start()
                    else:
                        pl.when(p == 0)(lambda: olocal(g, part, 1, hd).start())
                        pl.when(p > 0)(lambda: oremote(g, part, p, j, dest, 1, hd).start())

    def after(f, h, w, hw):
        @pl.when(f[4] == 1)
        def _():
            for e in range(tiles):
                finish(f[0], tiles * h + e)

        @pl.when(w[4] == 1)
        def _():
            for e in range(tiles):
                give_back(w[0], tiles * hw + e)

    bufs = ((sa, xa), (sb, xb))

    def nxt(f, h, e, par, masked):
        rows = (e + 1) * tq if masked else kb.shape[2]
        sx, xx = bufs[par]
        return qb[f[0], h, pl.ds(e * tq, tq), :], kb.at[f[1], f[2]], sx.at[e], xx.at[e], e * tq if masked else None, rows

    def step(fn, hn, f, h, parity):
        qs = f[0]
        for par in range(2):
            for m_cur in (False, True):
                for m_nxt in (False, True):
                    @pl.when((parity == par) & (f[3] == int(m_cur)) & (fn[3] == int(m_nxt)))
                    def _():
                        for e in range(tiles):
                            n = tiles * h + e
                            sx, xx = bufs[par]
                            keys = (e + 1) * tq if m_cur else kb.shape[2]
                            stage(c, nxt(fn, hn, e, 1 - par, m_nxt),
                                  (sx.at[e], xx.at[e], vb.at[f[1], f[2]], m.at[qs, n], l.at[qs, n], a.at[qs, n], keys))

    first = fields(I(0))
    begin(0)
    xwait(0, (2,), (0,))
    before(first)
    for e in range(tiles):
        stage(c, nxt(first, I(0), e, 0, True), None)

    @pl.loop(0, count)
    def _(u):
        f = fields(u)
        fn = fields(jnp.minimum(u + 1, count - 1))
        w = fields(jnp.maximum(u - 1, 0))
        w[4] = jnp.where(u > 0, w[4], 0)

        @pl.loop(0, f[5])
        def _(h):
            wrap = h == f[5] - 1
            pl.when(wrap & (u + 1 < count))(lambda: before(fn))
            step([jnp.where(wrap, p, q) for p, q in zip(fn, f)], jnp.where(wrap, fn[10], f[10] + h + 1), f, f[10] + h,
                 lax.rem(f[6] + h, I(2)))
            after(f, f[10] + h, [jnp.where(h == 0, p, q) for p, q in zip(w, f)],
                  jnp.where(h == 0, w[10] + w[5] - 1, f[10] + h - 1))

    for g in range(SLOTS):
        for part in range(2):
            for p in range(1, NX):
                for kind in range(3):
                    xcopy(g, kind, part, p, j, mod(j + p)).wait_send()
    end = fields(count - 1)
    for e in range(tiles):
        give_back(end[0], tiles * (end[10] + end[5] - 1) + e)
    for g in range(SLOTS):
        for s in range(NZ):
            @pl.when(goes_down(g) & (s >= z))
            def _():
                for ch in (s, TOP - s):
                    for d in zcopies(g, ch, -1, dsend):
                        d.wait_send()

            @pl.when((z < NZ - 1) & (s <= z))
            def _():
                for d in zcopies(g, s, 1, usend):
                    d.wait_send()

            if g == 1:
                @pl.when((z < FAR) & (s <= z))
                def _():
                    for d in zcopies(g, TOP - s, 1, usend):
                        d.wait_send()
        for part in range(2):
            def keep():
                olocal(g, part).wait()
                for p in range(1, NX):
                    oremote(g, part, p, j, mod(j + p)).wait_send()
                    oremote(g, part, p, mod(j - p), j).wait_recv()

            def given():
                for p in range(NX):
                    oremote(g, part, p, mod(j - p), j).wait_recv()

            if g == 1 and part == 1:
                pl.when(z == 0)(given)
                pl.when(z > 0)(keep)
            else:
                keep()

    @pl.when(z == 0)
    def _():
        for zz in SHARE:
            shift(zz).wait_send()

    for zz in SHARE:
        @pl.when(z == zz)
        def _():
            for p in range(NX):
                oremote(1, 1, p, j, mod(j + p), SHARE[zz][1], shifted=True).wait_send()


def solution(mesh):
    assert mesh.shape["cx"] == NX and mesh.shape["cy"] == NZ
    spec = P(("batch", "cy", "cx"), None, None)

    def local(q, k, v):
        t, h, d = q.shape
        pc = t // 2
        rows = NX * pc
        c = d ** -0.5 * math.log2(math.e)
        tq = 2 * pc
        tiles = rows // tq
        f32, bf = jnp.float32, jnp.bfloat16
        dma = pltpu.SemaphoreType.DMA
        ot = pl.pallas_call(
            functools.partial(kernel, c),
            out_shape=jax.ShapeDtypeStruct((h, t, d), bf),
            in_specs=[pl.BlockSpec(memory_space=pl.ANY)] * 3,
            out_specs=pl.BlockSpec(memory_space=pl.ANY),
            scratch_shapes=[
                pltpu.VMEM((5, GQ, rows, d), bf),
                pltpu.VMEM((SLOTS, 2 * NZ, rows, d), bf),
                pltpu.VMEM((SLOTS, 2 * NZ, d, rows), bf),
                pltpu.VMEM((5, GQ * tiles, 1, tq), f32),
                pltpu.VMEM((5, GQ * tiles, 8, tq), f32),
                pltpu.VMEM((5, GQ * tiles, d, tq), f32),
                pltpu.VMEM((5, GQ, rows, d), bf),
                pltpu.VMEM((tiles, rows, tq), f32),
                pltpu.VMEM((tiles, rows, tq), f32),
                pltpu.VMEM((tiles, 8, tq), f32),
                pltpu.VMEM((tiles, 8, tq), f32),
                dma((SLOTS, 3, 2, NX - 1)),
                dma((SLOTS, 3, 2, NX - 1)),
                dma((SLOTS, 3, 2)),
                dma((NZ - 1,)),
                dma((1,)),
                dma((SLOTS, 2 * NZ, 2)),
                dma((SLOTS, 2 * NZ, 2)),
                dma((SLOTS, 2 * NZ, 2)),
                dma((5, NX)),
                dma((4, NX)),
            ],
            compiler_params=pltpu.CompilerParams(
                collective_id=0, has_side_effects=True, vmem_limit_bytes=38 * 2**20),
        )(jnp.transpose(q, (1, 0, 2)), jnp.transpose(k, (1, 0, 2)), jnp.transpose(v, (1, 2, 0)))
        return jnp.transpose(ot, (1, 0, 2))

    return jax.shard_map(local, mesh=mesh, in_specs=(spec, spec, spec), out_specs=spec, check_vma=False)
```
